32 devices in a mesh: row: 8 (over y, x, core), col: 4 (over z).
Axes of the slice: x: 2, y: 2, z: 4, core: 2. Of those that a mesh axis runs over, the one named last changes fastest.
Arguments:
- signal: float32 [128, 128, 16, 256], P('row', 'col'), may hold values from -40 to 40, as said below
- start_frames: float32 [256, 32], replicated, may hold values from -6 to 6
- start_sends: float32 [16, 8], replicated, may hold values from -6 to 6
- start_rows: float32 [128, 64], replicated, may hold values from -6 to 6
- start_cols: float32 [128, 64], replicated, may hold values from -6 to 6
- rank_frames: int32 [1], replicated, may hold values from 16 to 32
- rank_sends: int32 [1], replicated, may hold values from 4 to 8
Outputs:
- filtered: float32 [128, 128, 16, 256], P('row', 'col')
The draws below stay inside these ranges and needn't reach their ends.
Inputs may be any that keep to these rules, and one draw needn't show every extreme that they name: `signal`: beamformed samples.
All inputs are finite; a program needn't handle non-finite values.
Results may differ from the reference program's by a relative error of at most 0.0003.
Values sent between devices are 32-bit elements; how exact they have to be, the bound alone decides.
No kernel may reach another device: no remote copies, remote signals or barrier semaphores. Data moves between devices by JAX's collectives and lax.ppermute only.
A program may use at most 128 MiB of HBM per device.

```python
import math
import jax
import jax.numpy as jnp
from jax import lax

NT = 256
NK = 16
TMAX = 32
KMAX = 8
RS = 64
ITERS = 2
CORE_W = 256
NR = 128
NC = 128


def cosine_modes(length):
    places = jnp.arange(length, dtype=jnp.float32)
    return jnp.cos(math.pi * (places[:, None] + 0.5) * places[None, :] / length) * math.sqrt(2.0 / length)


def slow_waves(key, length, count, first):
    places = jnp.arange(length, dtype=jnp.float32)
    phases = jax.random.uniform(key, (count,), jnp.float32, -math.pi, math.pi)
    freqs = jnp.arange(count, dtype=jnp.float32) + first
    return jnp.cos(2.0 * math.pi * places[:, None] * freqs[None, :] / length + phases[None, :]) * math.sqrt(2.0)


def draw_signal(key, part):
    keys = jax.random.split(jax.random.fold_in(key, 7331), 8)
    maps_count = 64
    row_modes = cosine_modes(NR)
    col_modes = cosine_modes(NC)
    row_decay = jnp.exp(-4.0 * jnp.arange(NR, dtype=jnp.float32) / NR)
    col_decay = jnp.exp(-4.0 * jnp.arange(NC, dtype=jnp.float32) / NC)
    coeffs = jax.random.normal(keys[0], (maps_count, NR, NC), jnp.float32)
    coeffs = coeffs * row_decay[None, :, None] * col_decay[None, None, :]
    half_maps = jnp.einsum('rj,qjc->qrc', row_modes, coeffs)
    maps = jnp.einsum('qrj,cj->qrc', half_maps, col_modes)
    frame_base = jnp.concatenate([slow_waves(keys[1], NT, 4, 1.0), jax.random.normal(keys[2], (NT, NT - 4), jnp.float32)], axis=1)
    frame_mix = frame_base * jnp.exp(-3.0 * jnp.arange(NT, dtype=jnp.float32) / NT)[None, :]
    send_base = jnp.concatenate([slow_waves(keys[3], NK, 2, 0.5), jax.random.normal(keys[4], (NK, NK - 2), jnp.float32)], axis=1)
    send_mix = send_base * jnp.exp(-2.0 * jnp.arange(NK, dtype=jnp.float32) / NK)[None, :]
    mixing = jax.random.normal(keys[5], (maps_count, NK, NT), jnp.float32)
    profiles = jnp.einsum('ka,qab,tb->qkt', send_mix, mixing, frame_mix)
    tissue = jnp.dot(maps.reshape(maps_count, -1).T, profiles.reshape(maps_count, -1))
    tissue = tissue.reshape(NR, NC, NK, NT)
    tissue = tissue * (4.0 / jnp.sqrt(jnp.mean(tissue * tissue)))
    noise = jax.random.truncated_normal(keys[7], -6.0, 6.0, (NR, NC, NK, NT), jnp.float32)
    signal = tissue + noise
    return jnp.clip(signal, -40.0, 40.0)


def scatter_about(key, shape, scale, bound, kind=jnp.bfloat16):
    drawn = jax.random.normal(key, shape, jnp.float32) * scale
    return jnp.minimum(jnp.maximum(drawn, -bound), bound).astype(kind)


def setup_inputs(seed: int = 0) -> dict:
    streams_of = jax.random.split(jax.random.key(seed), 8)
    signal = draw_signal(jax.random.fold_in(streams_of[7], 71), 0)
    start_frames = scatter_about(streams_of[1], (NT, TMAX), 1.0, 6.0, jnp.float32)
    start_sends = scatter_about(streams_of[2], (NK, KMAX), 1.0, 6.0, jnp.float32)
    start_rows = scatter_about(streams_of[3], (NR, RS), 1.0, 6.0, jnp.float32)
    start_cols = scatter_about(streams_of[4], (NC, RS), 1.0, 6.0, jnp.float32)
    rank_frames = jax.random.randint(streams_of[5], (1,), TMAX // 2, TMAX + 1).astype(jnp.int32)
    rank_sends = jax.random.randint(streams_of[6], (1,), KMAX // 2, KMAX + 1).astype(jnp.int32)
    return dict(signal=signal, start_frames=start_frames, start_sends=start_sends, start_rows=start_rows, start_cols=start_cols, rank_frames=rank_frames, rank_sends=rank_sends)


def orthonormal(gram, start):
    high = lax.Precision.HIGHEST
    basis = start
    for rounds in range(ITERS):
        image = jnp.dot(gram, basis, precision=high)
        inner = jnp.dot(image.T, image, precision=high)
        factor = jnp.linalg.cholesky(inner)
        basis = jax.scipy.linalg.solve_triangular(factor, image.T, lower=True).T
    return basis

def reference(signal, start_frames, start_sends, start_rows, start_cols, rank_frames, rank_sends):
    high = lax.Precision.HIGHEST
    total_rows, total_cols = (signal.shape[0], signal.shape[1])
    flattened = signal.reshape(-1, NT)
    blocks = signal.reshape(-1, NK, NT)
    gram_frames = jnp.dot(flattened.T, flattened, precision=high)
    gram_sends = jnp.einsum('pkt,pjt->kj', blocks, blocks, precision=high)
    keep_frames = (jnp.arange(TMAX, dtype=jnp.int32) < rank_frames[0]).astype(jnp.float32)
    keep_sends = (jnp.arange(KMAX, dtype=jnp.int32) < rank_sends[0]).astype(jnp.float32)
    basis_frames = orthonormal(gram_frames, start_frames) * keep_frames[None, :]
    basis_sends = orthonormal(gram_sends, start_sends) * keep_sends[None, :]
    reduced = jnp.dot(flattened, basis_frames, precision=high).reshape(-1, NK, TMAX)
    core = jnp.einsum('pkb,ka->pab', reduced, basis_sends, precision=high)
    unfolded = core.reshape(total_rows, -1)
    gram_rows = jnp.dot(unfolded, unfolded.T, precision=high)
    basis_rows = orthonormal(gram_rows, start_rows)
    second = jnp.dot(basis_rows.T, unfolded, precision=high).reshape(RS, total_cols, CORE_W)
    gram_cols = jnp.einsum('sce,sde->cd', second, second, precision=high)
    basis_cols = orthonormal(gram_cols, start_cols)
    third = jnp.einsum('cu,sce->sue', basis_cols, second, precision=high)
    back_cols = jnp.einsum('cu,sue->sce', basis_cols, third, precision=high)
    tissue_core = jnp.dot(basis_rows, back_cols.reshape(RS, -1), precision=high)
    tissue_core = tissue_core.reshape(-1, KMAX, TMAX)
    expanded = jnp.einsum('pab,ka->pkb', tissue_core, basis_sends, precision=high)
    tissue = jnp.dot(expanded.reshape(-1, TMAX), basis_frames.T, precision=high).reshape(signal.shape)
    return signal - tissue
```

```python
import functools

import jax
import jax.numpy as jnp
from jax import lax
from jax.experimental import pallas as pl
from jax.experimental.pallas import tpu as pltpu
from jax.sharding import PartitionSpec as P

ITERS = 2
LANES = 128
SUB = 8
HIGH = lax.Precision.HIGHEST
F32 = jnp.float32
BF16 = jnp.bfloat16
VMEM = pltpu.VMEM


NN = (((1,), (0,)), ((), ()))
NT = (((1,), (1,)), ((), ()))
TN = (((0,), (0,)), ((), ()))


def mm(a, b, dims):
    return lax.dot_general(a, b, dims, preferred_element_type=F32)


def mmf(a, b, dims):
    return lax.dot_general(a, b, dims, precision=HIGH, preferred_element_type=F32)


def split2(x):
    hi = x.astype(BF16)
    return hi, (x - hi.astype(F32)).astype(BF16)


def split3(x):
    hi = x.astype(BF16)
    rest = x - hi.astype(F32)
    mid = rest.astype(BF16)
    return hi, mid, (rest - mid.astype(F32)).astype(BF16)


def iota(shape, dim):
    return lax.broadcasted_iota(jnp.int32, shape, dim)


def whole(shape):
    return pl.BlockSpec(shape, lambda *_: (0,) * len(shape))


def gram_kernel(sends, pieces, x_ref, out_ref, acc_frames, acc_sends):
    step = pl.program_id(0)
    frames = x_ref.shape[1]
    group = acc_sends.shape[0]

    @pl.when(step == 0)
    def _():
        acc_frames[...] = jnp.zeros_like(acc_frames)
        acc_sends[...] = jnp.zeros_like(acc_sends)

    hi, lo = split2(x_ref[...])
    both = jnp.concatenate([hi, lo], axis=1)
    acc_frames[...] += mm(hi, both, TN)
    total_hh = acc_sends[:, :group]
    total_hl = acc_sends[:, group:]
    for at in range(0, x_ref.shape[0], group):
        h, l = hi[at : at + group], lo[at : at + group]
        total_hh += mm(h, h, NT)
        total_hl += mm(h, l, NT)
    acc_sends[:, :group] = total_hh
    acc_sends[:, group:] = total_hl

    @pl.when(step == pl.num_programs(0) - 1)
    def _():
        cross = acc_frames[:, frames:]
        gram = acc_frames[:, :frames] + (cross + cross.T)
        cross = acc_sends[:, group:]
        pair = acc_sends[:, :group] + (cross + cross.T)
        same = iota(pair.shape, 0) // sends == iota(pair.shape, 1) // sends
        pair = jnp.where(same, pair, 0.0)
        folded = pair[:sends]
        for at in range(sends, group, sends):
            folded = folded + pair[at : at + sends]
        pick = (iota((group, LANES), 0) % sends == iota((group, LANES), 1)).astype(F32)
        small = mmf(folded, pick, NN)
        parts = frames // LANES
        rows = sends // parts
        tile = jnp.concatenate([small[q * rows : (q + 1) * rows] for q in range(parts)], axis=1)
        piece = frames // pieces
        for q in range(pieces):
            out_ref[q, :piece] = gram[q * piece : (q + 1) * piece]
            out_ref[q, piece:] = tile


def signal_grams(flat, sends, pieces):
    rows, frames = flat.shape
    block = min(rows, 1024)
    group = min(block, 256)
    tail = sends * LANES // frames
    return pl.pallas_call(
        functools.partial(gram_kernel, sends, pieces),
        grid=(rows // block,),
        in_specs=[pl.BlockSpec((block, frames), lambda i: (i, 0))],
        out_specs=whole((pieces, frames // pieces + tail, frames)),
        out_shape=jax.ShapeDtypeStruct((pieces, frames // pieces + tail, frames), F32),
        scratch_shapes=[VMEM((frames, 2 * frames), F32), VMEM((group, 2 * group), F32)],
        name="signal_grams",
    )(flat)


def sweep(inner, image):
    count = inner.shape[0]
    blocks = count // SUB
    tiles = image.shape[1] // LANES
    a = [inner[SUB * i : SUB * (i + 1)] for i in range(blocks)]
    z = [
        [image[SUB * i : SUB * (i + 1), LANES * t : LANES * (t + 1)] for t in range(tiles)]
        for i in range(blocks)
    ]
    row = iota((SUB, LANES), 0)
    done = []
    for j in range(blocks):
        cols = [
            {i: jnp.broadcast_to(a[i][:, SUB * j + k : SUB * j + k + 1], (SUB, LANES)) for i in range(j, blocks)}
            for k in range(SUB)
        ]
        scale = jnp.zeros((SUB, LANES), F32)
        for k in range(SUB):
            pivot = jnp.broadcast_to(cols[k][j][k : k + 1], (SUB, LANES))
            inverse = 1.0 / pivot
            scale = jnp.where(row == k, lax.rsqrt(pivot), scale)
            a_row = jnp.broadcast_to(a[j][k : k + 1], (SUB, LANES)) * inverse
            z_row = [jnp.broadcast_to(t[k : k + 1], (SUB, LANES)) * inverse for t in z[j]]
            c_row = {
                q: jnp.broadcast_to(cols[q][j][k : k + 1], (SUB, LANES)) * inverse for q in range(k + 1, SUB)
            }
            for i in range(j, blocks):
                by = cols[k][i]
                if i == j:
                    by = jnp.where(row > k, by, 0.0)
                for q in range(k + 1, SUB):
                    cols[q][i] = cols[q][i] - by * c_row[q]
                if j + 1 < blocks:
                    a[i] = a[i] - by * a_row
                z[i] = [t - by * r for t, r in zip(z[i], z_row)]
        done.append([t * scale for t in z[j]])
    lines = [jnp.concatenate(d, axis=1) if tiles > 1 else d[0] for d in done]
    return jnp.concatenate(lines, axis=0) if blocks > 1 else lines[0]


def orthonormal(gram, start):
    basis = start
    for _ in range(ITERS):
        image = mmf(basis, gram, NN)
        count = image.shape[0]
        padded = jnp.concatenate([image, jnp.zeros((LANES - count, image.shape[1]), F32)], axis=0)
        basis = sweep(mmf(image, padded, NT), image)
    return basis


def small_bases_kernel(kmax, cols, gram_ref, tile_ref, sf_ref, ss_ref, rf_ref, rs_ref, frames_ref, spread_ref):
    frames = gram_ref.shape[1]
    tile = tile_ref[...]
    gram_s = jnp.concatenate([tile[:, LANES * q : LANES * (q + 1)] for q in range(frames // LANES)], axis=0)
    sends = gram_s.shape[0]
    gram_s = jnp.concatenate([gram_s, jnp.zeros((LANES - sends, LANES), F32)], axis=0)
    basis_f = orthonormal(gram_ref[...], sf_ref[...])
    basis_f = jnp.where(iota(basis_f.shape, 0) < rf_ref[0], basis_f, 0.0)
    frames_ref[...] = basis_f
    basis_s = orthonormal(gram_s, ss_ref[...])
    basis_s = jnp.where(iota(basis_s.shape, 0) < rs_ref[0], basis_s, 0.0)
    pick = (iota((kmax, kmax * cols), 0) == iota((kmax, kmax * cols), 1) // cols).astype(F32)
    spread_ref[...] = mmf(basis_s, pick, TN)[:sends]


def small_bases(gram, tile, start_frames, start_sends, rank_frames, rank_sends, cols):
    frames, tmax = start_frames.shape
    sends, kmax = start_sends.shape
    padded = jnp.pad(start_sends.T, ((0, 0), (0, LANES - sends)))
    full = lambda x: whole(x.shape)
    smem = pl.BlockSpec(memory_space=pltpu.SMEM)
    args = (gram, tile, start_frames.T, padded)
    return pl.pallas_call(
        functools.partial(small_bases_kernel, kmax, cols),
        in_specs=[full(x) for x in args] + [smem, smem],
        out_specs=[whole((tmax, frames)), whole((sends, kmax * cols))],
        out_shape=[jax.ShapeDtypeStruct((tmax, frames), F32), jax.ShapeDtypeStruct((sends, kmax * cols), F32)],
        name="small_bases",
    )(*args, rank_frames, rank_sends)


def mixing(spread, cols):
    sends, wide = spread.shape
    tall = jnp.broadcast_to(spread[None], (cols, sends, wide)).reshape(cols * sends, wide)
    same = iota(tall.shape, 0) // sends == iota(tall.shape, 1) % cols
    return jnp.where(same, tall, 0.0)


def core_kernel(cols, lanes, x_ref, basis_ref, spread_ref, out_ref, held, mix_ref, base_ref):
    step = pl.program_id(0)
    tmax = basis_ref.shape[0]

    @pl.when(step == 0)
    def _():
        for q, part in enumerate(split3(mixing(spread_ref[...], cols))):
            mix_ref[q] = part
        for q, part in enumerate(split3(basis_ref[...])):
            base_ref[q * tmax : (q + 1) * tmax] = part

    span = mix_ref.shape[1]
    rows = x_ref.shape[0] // span
    for q in range(rows):
        xh, xm, xl = split3(x_ref[q * span : (q + 1) * span])
        full = mm(base_ref[...], xh, NT)
        two = mm(base_ref[: 2 * tmax], xm, NT)
        one = mm(base_ref[:tmax], xl, NT)
        y = full[:tmax] + (full[tmax : 2 * tmax] + two[:tmax]) + (full[2 * tmax :] + two[tmax:] + one)
        stack = jnp.concatenate(split3(y), axis=0)
        full = mm(stack, mix_ref[0], NN)
        two = mm(stack[: 2 * tmax], mix_ref[1], NN)
        one = mm(stack[:tmax], mix_ref[2], NN)
        c = full[:tmax] + (full[tmax : 2 * tmax] + two[:tmax]) + (full[2 * tmax :] + two[tmax:] + one)
        for h in range(c.shape[1] // lanes):
            held[step * rows + q, h * tmax : (h + 1) * tmax] = c[:, h * lanes : (h + 1) * lanes]

    @pl.when(step == pl.num_programs(0) - 1)
    def _():
        for r in range(held.shape[0]):
            out_ref[:, r, :] = held[r]


def project(flat, basis, spread, rows_dev, cols, lanes):
    rows, frames = flat.shape
    tmax = basis.shape[0]
    sends, wide = spread.shape
    span = cols * sends
    per = 2 if rows_dev % 2 == 0 else 1
    high = wide * tmax // lanes
    return pl.pallas_call(
        functools.partial(core_kernel, cols, lanes),
        grid=(rows // (span * per),),
        in_specs=[
            pl.BlockSpec((span * per, frames), lambda i: (i, 0)),
            whole(basis.shape),
            whole(spread.shape),
        ],
        out_specs=whole((high, rows_dev, lanes)),
        out_shape=jax.ShapeDtypeStruct((high, rows_dev, lanes), F32),
        scratch_shapes=[
            VMEM((rows_dev, high, lanes), F32),
            VMEM((3, span, wide), BF16),
            VMEM((3 * tmax, frames), BF16),
        ],
        name="project",
    )(flat, basis, spread)


def block_of(ref, j, g):
    part = ref[:, j, g]
    return part.reshape(part.shape[0] * part.shape[1], part.shape[2])


def row_gram_kernel(m_ref, out_ref):
    total = None
    cross = None
    for j in range(m_ref.shape[1]):
        for g in range(m_ref.shape[2]):
            h, l = split2(block_of(m_ref, j, g))
            hh, hl = mm(h, h, NT), mm(h, l, NT)
            total = hh if total is None else total + hh
            cross = hl if cross is None else cross + hl
    out_ref[...] = total + (cross + cross.T)


def row_gram(m):
    rows = m.shape[0] * m.shape[3]
    return pl.pallas_call(
        row_gram_kernel, out_shape=jax.ShapeDtypeStruct((rows, rows), F32), name="row_gram"
    )(m)


def second_kernel(cols, gram_ref, start_ref, m_ref, basis_ref, second_ref, out_ref):
    basis = orthonormal(gram_ref[...], start_ref[...])
    basis_ref[...] = basis
    sections = m_ref.shape[1]
    low = m_ref.shape[4] // cols
    total = None
    for g in range(m_ref.shape[2]):
        for j in range(sections):
            t = mmf(block_of(m_ref, j, g), basis, (((0,), (1,)), ((), ())))
            for e in range(low):
                second_ref[g * low + e, j * cols : (j + 1) * cols] = t[e * cols : (e + 1) * cols]
        for e in range(low):
            s = second_ref[g * low + e]
            now = mmf(s, s, NT)
            total = now if total is None else total + now
    out_ref[...] = total


def second_stage(gram, start, m, cols):
    rows, kept = start.shape
    sections, groups, lanes = m.shape[1], m.shape[2], m.shape[4]
    low = lanes // cols
    wide = sections * cols
    return pl.pallas_call(
        functools.partial(second_kernel, cols),
        out_shape=[
            jax.ShapeDtypeStruct((kept, rows), F32),
            jax.ShapeDtypeStruct((groups * low, wide, kept), F32),
            jax.ShapeDtypeStruct((wide, wide), F32),
        ],
        name="second_stage",
    )(gram, start.T, m)


def third_kernel(cols, gram_ref, start_ref, basis_ref, second_ref, out_ref):
    basis_c = orthonormal(gram_ref[...], start_ref[...])
    project_c = mmf(basis_c, basis_c, TN)
    rows_t = basis_ref[...]
    sections = out_ref.shape[1]
    low = out_ref.shape[4] // cols
    for g in range(out_ref.shape[2]):
        kept = [mmf(project_c, second_ref[g * low + e], NN) for e in range(low)]
        for j in range(sections):
            part = jnp.concatenate([k[j * cols : (j + 1) * cols] for k in kept], axis=0)
            t = mmf(rows_t, part, (((0,), (1,)), ((), ())))
            out_ref[:, j, g] = t.reshape(out_ref.shape[0], out_ref.shape[3], out_ref.shape[4])


def third_stage(gram, start, basis, second, shape, cols):
    return pl.pallas_call(
        functools.partial(third_kernel, cols),
        out_shape=jax.ShapeDtypeStruct(shape, F32),
        name="third_stage",
    )(gram, start.T, basis, second)


def expand_kernel(cols, x_ref, t_ref, basis_ref, spread_ref, out_ref, held, mix_ref, base_ref):
    step = pl.program_id(0)
    tmax = basis_ref.shape[0]

    @pl.when(step == 0)
    def _():
        for q, part in enumerate(split3(mixing(spread_ref[...], cols))):
            mix_ref[q] = part
        hi, mid, lo = split3(basis_ref[...])
        for q, part in enumerate((hi, mid, lo, hi, mid, hi)):
            base_ref[q * tmax : (q + 1) * tmax] = part
        for r in range(held.shape[0]):
            held[r] = t_ref[:, r, :]

    span = mix_ref.shape[1]
    rows = x_ref.shape[0] // span
    for q in range(rows):
        t = held[step * rows + q]
        t = jnp.concatenate([t[h * tmax : (h + 1) * tmax] for h in range(t.shape[0] // tmax)], axis=1)
        stack = jnp.concatenate(split3(t), axis=0)
        full = mm(stack, mix_ref[0], NT)
        two = mm(stack[: 2 * tmax], mix_ref[1], NT)
        one = mm(stack[:tmax], mix_ref[2], NT)
        z = full[:tmax] + (full[tmax : 2 * tmax] + two[:tmax]) + (full[2 * tmax :] + two[tmax:] + one)
        hi, mid, lo = split3(z)
        tall = jnp.concatenate([hi, hi, hi, mid, mid, lo], axis=0)
        tissue = mm(tall, base_ref[...], TN)
        at = slice(q * span, (q + 1) * span)
        out_ref[at] = x_ref[at] - tissue


def expand(flat, t, basis, spread, cols):
    rows, frames = flat.shape
    tmax = basis.shape[0]
    sends, wide = spread.shape
    high, rows_dev, lanes = t.shape
    span = cols * sends
    per = 2 if rows_dev % 2 == 0 else 1
    block = pl.BlockSpec((span * per, frames), lambda i: (i, 0))
    return pl.pallas_call(
        functools.partial(expand_kernel, cols),
        grid=(rows // (span * per),),
        in_specs=[block, whole(t.shape), whole(basis.shape), whole(spread.shape)],
        out_specs=block,
        out_shape=jax.ShapeDtypeStruct(flat.shape, F32),
        scratch_shapes=[
            VMEM((rows_dev, high, lanes), F32),
            VMEM((3, span, wide), BF16),
            VMEM((6 * tmax, frames), BF16),
        ],
        name="expand",
    )(flat, t, basis, spread)


def shifted(x, axis, by, size):
    return lax.ppermute(x, axis, [(i, (i + by) % size) for i in range(size)])


def exchange_sum(x, axis, size, stride=1):
    total = x
    for by in range(stride, size, stride):
        total = total + shifted(x, axis, by, size)
    return total


def sum_all(x, rows, cols):
    if rows % 2 or rows < 4:
        return exchange_sum(exchange_sum(x, "row", rows), "col", cols)
    pairs = [(i, i ^ 1) for i in range(rows)]
    side = lax.axis_index("row") % 2
    half = x.shape[0] // 2
    mine = lax.dynamic_slice_in_dim(x, side * half, half, 0)
    other = lax.dynamic_slice_in_dim(x, (1 - side) * half, half, 0)
    mine = mine + lax.ppermute(other, "row", pairs)
    mine = exchange_sum(mine, "row", rows, 2)
    mine = exchange_sum(mine, "col", cols)
    other = lax.ppermute(mine, "row", pairs)
    first = jnp.where(side == 0, mine, other)
    last = jnp.where(side == 0, other, mine)
    return jnp.concatenate([first, last], axis=0)


def local(rows, cols, signal, start_frames, start_sends, start_rows, start_cols, rank_frames, rank_sends):
    rows_dev, cols_dev, sends, frames = signal.shape
    kmax, tmax = start_sends.shape[1], start_frames.shape[1]
    devices = rows * cols
    flat = signal.reshape(-1, frames)

    pieces = signal_grams(flat, sends, rows)
    piece = frames // rows
    mine = lax.all_to_all(pieces, "row", 0, 0).sum(0)
    mine = exchange_sum(mine, "col", cols)
    gram_frames = lax.all_gather(mine[:piece], "row", axis=0, tiled=True)
    basis, spread = small_bases(
        gram_frames, mine[piece:], start_frames, start_sends, rank_frames, rank_sends, cols_dev
    )

    low = min(LANES // cols_dev, kmax * tmax // devices, kmax)
    lanes = low * cols_dev
    core = project(flat, basis, spread, rows_dev, cols_dev, lanes)
    groups = core.shape[0] // devices
    core = core.reshape(devices, groups, rows_dev, lanes)
    m = lax.all_to_all(core, ("row", "col"), 0, 0).reshape(rows, cols, groups, rows_dev, lanes)

    gram_rows = sum_all(row_gram(m), rows, cols)
    basis_rows, second, gram_cols = second_stage(gram_rows, start_rows, m, cols_dev)
    gram_cols = sum_all(gram_cols, rows, cols)
    t = third_stage(gram_cols, start_cols, basis_rows, second, m.shape, cols_dev)

    t = t.reshape(devices, groups, rows_dev, lanes)
    t = lax.all_to_all(t, ("row", "col"), 0, 0).reshape(devices * groups, rows_dev, lanes)
    return expand(flat, t, basis, spread, cols_dev).reshape(signal.shape)


def solution(mesh):
    rows, cols = mesh.shape["row"], mesh.shape["col"]
    return jax.shard_map(
        functools.partial(local, rows, cols),
        mesh=mesh,
        in_specs=(P("row", "col", None, None), P(), P(), P(), P(), P(), P()),
        out_specs=P("row", "col", None, None),
        check_vma=False,
    )
```

```python
import functools

import jax
import jax.numpy as jnp
from jax import lax
from jax.experimental import pallas as pl
from jax.experimental.pallas import tpu as pltpu
from jax.sharding import PartitionSpec as P

ITERS = 2
LANES = 128
SUB = 8
HIGH = lax.Precision.HIGHEST
F32 = jnp.float32
BF16 = jnp.bfloat16
VMEM = pltpu.VMEM


NN = (((1,), (0,)), ((), ()))
NT = (((1,), (1,)), ((), ()))
TN = (((0,), (0,)), ((), ()))


def mm(a, b, dims):
    return lax.dot_general(a, b, dims, preferred_element_type=F32)


def mmf(a, b, dims):
    return lax.dot_general(a, b, dims, precision=HIGH, preferred_element_type=F32)


def split2(x):
    hi = x.astype(BF16)
    return hi, (x - hi.astype(F32)).astype(BF16)


def split3(x):
    hi = x.astype(BF16)
    rest = x - hi.astype(F32)
    mid = rest.astype(BF16)
    return hi, mid, (rest - mid.astype(F32)).astype(BF16)


def iota(shape, dim):
    return lax.broadcasted_iota(jnp.int32, shape, dim)


def params(mib=24):
    return pltpu.CompilerParams(vmem_limit_bytes=mib * 2**20)


VSPEC = pl.BlockSpec(memory_space=VMEM)


def in_vmem(x):
    return pltpu.with_memory_space_constraint(x, VMEM)


def mm2(a, b, dims_last):
    (ah, al), (bh, bl) = a, b
    return mm(ah, bh, dims_last) + (mm(ah, bl, dims_last) + mm(al, bh, dims_last))


def whole(shape):
    return pl.BlockSpec(shape, lambda *_: (0,) * len(shape))


def pack(square):
    n = square.shape[0]
    h = n // 2
    top, low = square[:h], square[h:]
    row, lane = iota((h, n), 0), iota((h, n), 1)
    turned = pltpu.roll(low, h, 1)
    body = jnp.where(lane < row, turned, top)
    diag = jnp.sum(jnp.where(lane == row + h, low, 0.0), axis=0, keepdims=True)
    tail = jnp.where(iota((SUB, n), 0) == 0, jnp.broadcast_to(diag, (SUB, n)), 0.0)
    return body, tail


def unpack(body, tail):
    h, n = body.shape
    row, lane = iota((h, n), 0), iota((h, n), 1)
    flip = body.T
    first, last = flip[:h], flip[h:]
    if h % LANES:
        zeros = jnp.zeros((h, n - h), F32)
        first, last = jnp.concatenate([first, zeros], axis=1), jnp.concatenate([last, zeros], axis=1)
    else:
        first, last = jnp.concatenate([first, first], axis=1), jnp.concatenate([last, last], axis=1)
    top = jnp.where(lane < row, first, body)
    corner = pltpu.roll(jnp.where(lane < row, body, first), h, 1)
    corner = jnp.where(lane == row + h, jnp.broadcast_to(tail[:1], (h, n)), corner)
    return jnp.concatenate([top, jnp.where(lane < h, last, corner)], axis=0)


def gram_kernel(sends, x_ref, side_ref, mine_ref, other_ref, acc_frames, acc_sends):
    step = pl.program_id(0)
    frames = x_ref.shape[1]
    group = acc_sends.shape[0]

    @pl.when(step == 0)
    def _():
        acc_frames[...] = jnp.zeros_like(acc_frames)
        acc_sends[...] = jnp.zeros_like(acc_sends)

    hi, lo = split2(x_ref[...])
    acc_frames[...] += mm(hi, jnp.concatenate([hi, lo], axis=1), TN)
    total = acc_sends[...]
    for at in range(0, x_ref.shape[0], group):
        h, l = hi[at : at + group], lo[at : at + group]
        total += mm(h, jnp.concatenate([h, l], axis=0), NT)
    acc_sends[...] = total

    @pl.when(step == pl.num_programs(0) - 1)
    def _():
        cross = acc_frames[:, frames:]
        body, tail = pack(acc_frames[:, :frames] + (cross + cross.T))
        cross = acc_sends[:, group:]
        pair = acc_sends[:, :group] + (cross + cross.T)
        same = iota(pair.shape, 0) // sends == iota(pair.shape, 1) // sends
        pair = jnp.where(same, pair, 0.0)
        folded = pair[:sends]
        for at in range(sends, group, sends):
            folded = folded + pair[at : at + sends]
        half = sends // 2
        pick = (iota((group, LANES), 0) % sends == iota((group, LANES), 1)).astype(F32)
        small = mmf(folded, pick, NN)
        small = small[:half] + pltpu.roll(small[half:], sends, 1)
        side = side_ref[0]
        for ref, at in ((mine_ref, side), (other_ref, 1 - side)):
            left = at == 0
            ref[: body.shape[0]] = jnp.where(left, body[:, :LANES], body[:, LANES:])
            ref[body.shape[0] :] = jnp.where(left, tail[:, :LANES] + small, tail[:, LANES:])


def signal_grams(flat, sends, side):
    rows, frames = flat.shape
    block = min(rows, 1024)
    group = LANES
    shape = (frames // 2 + SUB, LANES)
    return pl.pallas_call(
        functools.partial(gram_kernel, sends),
        grid=(rows // block,),
        in_specs=[pl.BlockSpec((block, frames), lambda i: (i, 0)), pl.BlockSpec(memory_space=pltpu.SMEM)],
        out_specs=[whole(shape), whole(shape)],
        out_shape=[jax.ShapeDtypeStruct(shape, F32)] * 2,
        scratch_shapes=[VMEM((frames, 2 * frames), F32), VMEM((group, 2 * group), F32)],
        compiler_params=params(),
        name="signal_grams",
    )(flat, side)


def sweep(inner, image):
    count = inner.shape[0]
    blocks = count // SUB
    tiles = image.shape[1] // LANES
    a = [inner[SUB * i : SUB * (i + 1)] for i in range(blocks)]
    z = [
        [image[SUB * i : SUB * (i + 1), LANES * t : LANES * (t + 1)] for t in range(tiles)]
        for i in range(blocks)
    ]
    row = iota((SUB, LANES), 0)
    done = []
    for j in range(blocks):
        cols = [
            {i: jnp.broadcast_to(a[i][:, SUB * j + k : SUB * j + k + 1], (SUB, LANES)) for i in range(j, blocks)}
            for k in range(SUB)
        ]
        scale = jnp.zeros((SUB, LANES), F32)
        for k in range(SUB):
            pivot = jnp.broadcast_to(cols[k][j][k : k + 1], (SUB, LANES))
            inverse = 1.0 / pivot
            scale = jnp.where(row == k, lax.rsqrt(pivot), scale)
            a_row = jnp.broadcast_to(a[j][k : k + 1], (SUB, LANES)) * inverse
            z_row = [jnp.broadcast_to(t[k : k + 1], (SUB, LANES)) * inverse for t in z[j]]
            c_row = {
                q: jnp.broadcast_to(cols[q][j][k : k + 1], (SUB, LANES)) * inverse for q in range(k + 1, SUB)
            }
            for i in range(j, blocks):
                by = cols[k][i]
                if i == j:
                    by = jnp.where(row > k, by, 0.0)
                for q in range(k + 1, SUB):
                    cols[q][i] = cols[q][i] - by * c_row[q]
                if j + 1 < blocks:
                    a[i] = a[i] - by * a_row
                z[i] = [t - by * r for t, r in zip(z[i], z_row)]
        done.append([t * scale for t in z[j]])
    lines = [jnp.concatenate(d, axis=1) if tiles > 1 else d[0] for d in done]
    return jnp.concatenate(lines, axis=0) if blocks > 1 else lines[0]


def orthonormal(gram, start):
    def body(_, basis):
        image = mmf(basis, gram, NN)
        count = image.shape[0]
        padded = jnp.concatenate([image, jnp.zeros((LANES - count, image.shape[1]), F32)], axis=0)
        return sweep(mmf(image, padded, NT), image)

    return lax.fori_loop(0, ITERS, body, start)


def small_bases_kernel(
    kmax, cols, sends, mine_ref, other_ref, side_ref, sf_ref, ss_ref, rf_ref, rs_ref, frames_ref, spread_ref
):
    h = mine_ref.shape[0] - SUB
    left = side_ref[0] == 0
    mine, other = mine_ref[...], other_ref[...]
    first, last = jnp.where(left, mine, other), jnp.where(left, other, mine)
    gram_f = unpack(jnp.concatenate([first[:h], last[:h]], axis=1), jnp.concatenate([first[h:], last[h:]], axis=1))
    small = first[h:]
    lane = iota(small.shape, 1)
    gram_s = jnp.concatenate(
        [
            jnp.where(lane < sends, small, 0.0),
            jnp.where(lane < sends, pltpu.roll(small, LANES - sends, 1), 0.0),
            jnp.zeros((LANES - sends, LANES), F32),
        ],
        axis=0,
    )

    def body(_, bases):
        images = [mmf(basis, gram, NN) for basis, gram in zip(bases, (gram_f, gram_s))]
        inners = [
            mmf(i, jnp.concatenate([i, jnp.zeros((LANES - i.shape[0], i.shape[1]), F32)], axis=0), NT) for i in images
        ]
        return tuple(sweep(n, i) for n, i in zip(inners, images))

    basis_f, basis_s = lax.fori_loop(0, ITERS, body, (sf_ref[...], ss_ref[...]))
    frames_ref[...] = jnp.where(iota(basis_f.shape, 0) < rf_ref[0], basis_f, 0.0)
    basis_s = jnp.where(iota(basis_s.shape, 0) < rs_ref[0], basis_s, 0.0)
    pick = (iota((kmax, kmax * cols), 0) == iota((kmax, kmax * cols), 1) // cols).astype(F32)
    spread_ref[...] = mmf(basis_s, pick, TN)[:sends]


def small_bases(mine, other, side, start_frames, start_sends, rank_frames, rank_sends, cols):
    frames, tmax = start_frames.shape
    sends, kmax = start_sends.shape
    padded = jnp.pad(start_sends.T, ((0, 0), (0, LANES - sends)))
    smem = pl.BlockSpec(memory_space=pltpu.SMEM)
    return pl.pallas_call(
        functools.partial(small_bases_kernel, kmax, cols, sends),
        in_specs=[VSPEC, VSPEC, smem, VSPEC, VSPEC, smem, smem],
        out_specs=[VSPEC, VSPEC],
        out_shape=[jax.ShapeDtypeStruct((tmax, frames), F32), jax.ShapeDtypeStruct((sends, kmax * cols), F32)],
        compiler_params=params(),
        name="small_bases",
    )(mine, other, side, start_frames.T, padded, rank_frames, rank_sends)


def mixing(spread, cols):
    sends, wide = spread.shape
    tall = jnp.broadcast_to(spread[None], (cols, sends, wide)).reshape(cols * sends, wide)
    same = iota(tall.shape, 0) // sends == iota(tall.shape, 1) % cols
    return jnp.where(same, tall, 0.0)


def core_kernel(lanes, cols, per, x_ref, basis_ref, spread_ref, out_ref, held, mix_ref):
    tmax = basis_ref.shape[0]
    mix_ref[0], mix_ref[1] = split2(mixing(spread_ref[...], cols))
    bh, bl = split2(basis_ref[...])
    base = jnp.concatenate([bh, bl], axis=0)
    span = mix_ref.shape[1]

    def body(step, carry):
        his, los = [], []
        for q in range(per):
            at = pl.multiple_of((step * per + q) * span, span)
            xh, xl = split2(x_ref[pl.ds(at, span), :])
            both = mm(base, xh, NT)
            h, l = split2(both[:tmax] + (both[tmax:] + mm(bh, xl, NT)))
            his.append(h)
            los.append(l)
        rows = per * tmax
        stack = jnp.concatenate(his + los, axis=0)
        both = mm(stack, mix_ref[0], NN)
        c = both[:rows] + (both[rows:] + mm(stack[:rows], mix_ref[1], NN))
        for q in range(per):
            for h in range(c.shape[1] // lanes):
                held[step * per + q, h * tmax : (h + 1) * tmax] = c[
                    q * tmax : (q + 1) * tmax, h * lanes : (h + 1) * lanes
                ]
        return carry

    lax.fori_loop(0, held.shape[0] // per, body, 0)
    for r in range(held.shape[0]):
        out_ref[:, r, :] = held[r]


def project(flat, basis, spread, rows_dev, cols, lanes):
    frames = flat.shape[1]
    tmax = basis.shape[0]
    sends, wide = spread.shape
    span = cols * sends
    per = 2 if rows_dev % 2 == 0 else 1
    high = wide * tmax // lanes
    return pl.pallas_call(
        functools.partial(core_kernel, lanes, cols, per),
        in_specs=[VSPEC] * 3,
        out_specs=VSPEC,
        out_shape=jax.ShapeDtypeStruct((high, rows_dev, lanes), F32),
        scratch_shapes=[VMEM((rows_dev, high, lanes), F32), VMEM((2, span, wide), BF16)],
        compiler_params=params(),
        name="project",
    )(flat, basis, spread)


def block_of(ref, j, g):
    part = ref[:, j, g]
    return part.reshape(part.shape[0] * part.shape[1], part.shape[2])


def row_gram_kernel(m_ref, out_ref):
    total = None
    cross = None
    for j in range(m_ref.shape[1]):
        for g in range(m_ref.shape[2]):
            h, l = split2(block_of(m_ref, j, g))
            hh, hl = mm(h, h, NT), mm(h, l, NT)
            total = hh if total is None else total + hh
            cross = hl if cross is None else cross + hl
    put(out_ref, total + (cross + cross.T))


def put(ref, square):
    body, tail = pack(square)
    ref[: body.shape[0]] = body
    ref[body.shape[0] :] = tail


def get(ref):
    h = ref.shape[0] - SUB
    return unpack(ref[:h], ref[h:])


def row_gram(m):
    rows = m.shape[0] * m.shape[3]
    return pl.pallas_call(
        row_gram_kernel,
        in_specs=[VSPEC],
        out_specs=VSPEC,
        out_shape=jax.ShapeDtypeStruct((rows // 2 + SUB, rows), F32),
        compiler_params=params(),
        name="row_gram",
    )(m)


def second_kernel(cols, gram_ref, start_ref, m_ref, basis_ref, second_ref, out_ref):
    basis = orthonormal(get(gram_ref), start_ref[...])
    basis_ref[...] = basis
    uh, ul = split2(basis)
    twice = jnp.concatenate([uh, uh], axis=1)
    sections = m_ref.shape[1]
    low = m_ref.shape[4] // cols
    total = None
    cross = None
    contract = (((0,), (1,)), ((), ()))
    for g in range(m_ref.shape[2]):
        for j in range(sections):
            h, l = split2(block_of(m_ref, j, g))
            t = mm(jnp.concatenate([h, l], axis=0), twice, contract) + mm(h, ul, contract)
            for e in range(low):
                second_ref[g * low + e, j * cols : (j + 1) * cols] = t[e * cols : (e + 1) * cols]
        for e in range(low):
            h, l = split2(second_ref[g * low + e])
            hh, hl = mm(h, h, NT), mm(h, l, NT)
            total = hh if total is None else total + hh
            cross = hl if cross is None else cross + hl
    put(out_ref, total + (cross + cross.T))


def second_stage(gram, start, m, cols):
    rows, kept = start.shape
    sections, groups, lanes = m.shape[1], m.shape[2], m.shape[4]
    low = lanes // cols
    wide = sections * cols
    return pl.pallas_call(
        functools.partial(second_kernel, cols),
        in_specs=[VSPEC] * 3,
        out_specs=[VSPEC] * 3,
        out_shape=[
            jax.ShapeDtypeStruct((kept, rows), F32),
            jax.ShapeDtypeStruct((groups * low, wide, kept), F32),
            jax.ShapeDtypeStruct((wide // 2 + SUB, wide), F32),
        ],
        compiler_params=params(),
        name="second_stage",
    )(gram, start.T, m)


def third_kernel(cols, gram_ref, start_ref, basis_ref, second_ref, out_ref):
    basis_c = orthonormal(get(gram_ref), start_ref[...])
    ph, pl_ = split2(mmf(basis_c, basis_c, TN))
    twice = jnp.concatenate([ph, ph], axis=1)
    rows_t = split2(basis_ref[...].T)
    sections = out_ref.shape[1]
    low = out_ref.shape[4] // cols
    for g in range(out_ref.shape[2]):
        kept = []
        for e in range(low):
            h, l = split2(second_ref[g * low + e])
            kept.append(split2(mm(twice, jnp.concatenate([h, l], axis=0), NN) + mm(pl_, h, NN)))
        for j in range(sections):
            part = [
                jnp.concatenate([k[w][j * cols : (j + 1) * cols] for k in kept], axis=0) for w in range(2)
            ]
            t = mm2(rows_t, part, NT)
            out_ref[:, j, g] = t.reshape(out_ref.shape[0], out_ref.shape[3], out_ref.shape[4])


def third_stage(gram, start, basis, second, shape, cols):
    return pl.pallas_call(
        functools.partial(third_kernel, cols),
        in_specs=[VSPEC] * 4,
        out_specs=VSPEC,
        out_shape=jax.ShapeDtypeStruct(shape, F32),
        compiler_params=params(),
        name="third_stage",
    )(gram, start.T, basis, second)


def expand_kernel(cols, per, x_ref, t_ref, basis_ref, spread_ref, out_ref, held, mix_ref, base_ref):
    step = pl.program_id(0)
    tmax = basis_ref.shape[0]

    @pl.when(step == 0)
    def _():
        hi, lo = split2(mixing(spread_ref[...], cols))
        mix_ref[0], mix_ref[1] = hi.T, lo.T
        hi, lo = split2(basis_ref[...])
        for q, part in enumerate((hi, lo, hi)):
            base_ref[q * tmax : (q + 1) * tmax] = part
        for r in range(held.shape[0]):
            held[r] = t_ref[:, r, :]

    span = mix_ref.shape[2]
    tiles = []
    for q in range(per):
        t = held[step * per + q]
        tiles.append(jnp.concatenate([t[h * tmax : (h + 1) * tmax] for h in range(t.shape[0] // tmax)], axis=1))
    hi, lo = split2(jnp.concatenate(tiles, axis=0))
    rows = per * tmax
    both = mm(jnp.concatenate([hi, lo], axis=0), mix_ref[0], NN)
    zh, zl = split2(both[:rows] + (both[rows:] + mm(hi, mix_ref[1], NN)))
    for q in range(per):
        h, l = zh[q * tmax : (q + 1) * tmax], zl[q * tmax : (q + 1) * tmax]
        tissue = mm(jnp.concatenate([h, h, l], axis=0), base_ref[...], TN)
        at = pl.multiple_of((step * per + q) * span, span)
        out_ref[q * span : (q + 1) * span] = x_ref[pl.ds(at, span), :] - tissue


def expand(flat, t, basis, spread, cols):
    rows, frames = flat.shape
    tmax = basis.shape[0]
    sends, wide = spread.shape
    high, rows_dev, lanes = t.shape
    span = cols * sends
    per = 2 if rows_dev % 2 == 0 else 1
    return pl.pallas_call(
        functools.partial(expand_kernel, cols, per),
        grid=(rows // (span * per),),
        in_specs=[VSPEC] * 4,
        out_specs=pl.BlockSpec((span * per, frames), lambda i: (i, 0)),
        out_shape=jax.ShapeDtypeStruct(flat.shape, F32),
        scratch_shapes=[
            VMEM((rows_dev, high, lanes), F32),
            VMEM((2, wide, span), BF16),
            VMEM((3 * tmax, frames), BF16),
        ],
        compiler_params=params(),
        name="expand",
    )(flat, t, basis, spread)


def shifted(x, axis, by, size):
    return lax.ppermute(x, axis, [(i, (i + by) % size) for i in range(size)])


def exchange_sum(x, axis, size, stride=1):
    total = x
    for by in range(stride, size, stride):
        total = total + shifted(x, axis, by, size)
    return total


def sum_all(x, rows, cols):
    if rows % 2 == 0 and rows > 2:
        x = x + lax.ppermute(x, "row", [(i, i ^ 1) for i in range(rows)])
        x = exchange_sum(x, "row", rows, 2)
    else:
        x = exchange_sum(x, "row", rows)
    return exchange_sum(x, "col", cols)


def sum_halves(mine, other, rows, cols):
    pairs = [(i, i ^ 1) for i in range(rows)]
    mine = mine + lax.ppermute(other, "row", pairs)
    mine = exchange_sum(mine, "row", rows, 2)
    mine = exchange_sum(mine, "col", cols)
    return mine, lax.ppermute(mine, "row", pairs)


def local(rows, cols, signal, start_frames, start_sends, start_rows, start_cols, rank_frames, rank_sends):
    rows_dev, cols_dev, sends, frames = signal.shape
    kmax, tmax = start_sends.shape[1], start_frames.shape[1]
    devices = rows * cols
    flat = signal.reshape(-1, frames)
    side = (lax.axis_index("row") % 2).astype(jnp.int32).reshape(1)

    mine, other = sum_halves(*signal_grams(flat, sends, side), rows, cols)
    basis, spread = small_bases(
        mine, other, side, start_frames, start_sends, rank_frames, rank_sends, cols_dev
    )

    low = min(LANES // cols_dev, kmax * tmax // devices, kmax)
    lanes = low * cols_dev
    near = in_vmem(flat)
    core = project(near, basis, spread, rows_dev, cols_dev, lanes)
    groups = core.shape[0] // devices
    core = core.reshape(devices, groups, rows_dev, lanes)
    m = lax.all_to_all(core, ("row", "col"), 0, 0).reshape(rows, cols, groups, rows_dev, lanes)

    gram_rows = sum_all(row_gram(m), rows, cols)
    basis_rows, second, gram_cols = second_stage(gram_rows, start_rows, m, cols_dev)
    gram_cols = sum_all(gram_cols, rows, cols)
    t = third_stage(gram_cols, start_cols, basis_rows, second, m.shape, cols_dev)

    t = t.reshape(devices, groups, rows_dev, lanes)
    t = lax.all_to_all(t, ("row", "col"), 0, 0).reshape(devices * groups, rows_dev, lanes)
    return expand(near, t, basis, spread, cols_dev).reshape(signal.shape)


def solution(mesh):
    rows, cols = mesh.shape["row"], mesh.shape["col"]
    return jax.shard_map(
        functools.partial(local, rows, cols),
        mesh=mesh,
        in_specs=(P("row", "col", None, None), P(), P(), P(), P(), P(), P()),
        out_specs=P("row", "col", None, None),
        check_vma=False,
    )
```

```python
import functools

import jax
import jax.numpy as jnp
from jax import lax
from jax.experimental import pallas as pl
from jax.experimental.pallas import tpu as pltpu
from jax.sharding import PartitionSpec as P


ITERS = 2
LANES = 128
SUB = 8
HIGH = lax.Precision.HIGHEST
F32 = jnp.float32
BF16 = jnp.bfloat16
VMEM = pltpu.VMEM


NN = (((1,), (0,)), ((), ()))
NT = (((1,), (1,)), ((), ()))
TN = (((0,), (0,)), ((), ()))


def mm(a, b, dims):
    return lax.dot_general(a, b, dims, preferred_element_type=F32)


def mmf(a, b, dims):
    return lax.dot_general(a, b, dims, precision=HIGH, preferred_element_type=F32)


def split2(x):
    hi = x.astype(BF16)
    return hi, (x - hi.astype(F32)).astype(BF16)


def iota(shape, dim):
    return lax.broadcasted_iota(jnp.int32, shape, dim)


def params(mib=24):
    return pltpu.CompilerParams(vmem_limit_bytes=mib * 2**20)


VSPEC = pl.BlockSpec(memory_space=VMEM)


def in_vmem(x):
    return pltpu.with_memory_space_constraint(x, VMEM)


def mm2(a, b, dims_last):
    (ah, al), (bh, bl) = a, b
    return mm(ah, bh, dims_last) + (mm(ah, bl, dims_last) + mm(al, bh, dims_last))


def pack(square):
    n = square.shape[0]
    h = n // 2
    top, low = square[:h], square[h:]
    row, lane = iota((h, n), 0), iota((h, n), 1)
    turned = pltpu.roll(low, h, 1)
    body = jnp.where(lane < row, turned, top)
    diag = jnp.sum(jnp.where(lane == row + h, low, 0.0), axis=0, keepdims=True)
    tail = jnp.where(iota((SUB, n), 0) == 0, jnp.broadcast_to(diag, (SUB, n)), 0.0)
    return body, tail


def unpack(body, tail):
    h, n = body.shape
    row, lane = iota((h, n), 0), iota((h, n), 1)
    flip = body.T
    first, last = flip[:h], flip[h:]
    if h % LANES:
        zeros = jnp.zeros((h, n - h), F32)
        first, last = jnp.concatenate([first, zeros], axis=1), jnp.concatenate([last, zeros], axis=1)
    else:
        first, last = jnp.concatenate([first, first], axis=1), jnp.concatenate([last, last], axis=1)
    top = jnp.where(lane < row, first, body)
    corner = pltpu.roll(jnp.where(lane < row, body, first), h, 1)
    corner = jnp.where(lane == row + h, jnp.broadcast_to(tail[:1], (h, n)), corner)
    return jnp.concatenate([top, jnp.where(lane < h, last, corner)], axis=0)


def gram_kernel(sends, block, ahead, x_ref, side_ref, col_ref, near_ref, mine_ref, other_ref, acc_frames, acc_sends, sems):
    frames = x_ref.shape[1]
    group = acc_sends.shape[0]
    steps = x_ref.shape[0] // block

    def copy(step):
        at = pl.ds(pl.multiple_of(step * block, block), block)
        return pltpu.make_async_copy(x_ref.at[at, :], near_ref.at[at, :], sems.at[step])

    for step in range(min(ahead, steps)):
        copy(step).start()
    acc_frames[...] = jnp.zeros_like(acc_frames)
    acc_sends[...] = jnp.zeros_like(acc_sends)

    def body(step, carry):
        copy(step).wait()

        @pl.when(step + ahead < steps)
        def _():
            copy(step + ahead).start()

        hi, lo = split2(near_ref[pl.ds(pl.multiple_of(step * block, block), block), :])
        acc_frames[...] += mm(hi, jnp.concatenate([hi, lo], axis=1), TN)
        total = acc_sends[...]
        for at in range(0, block, group):
            h, l = hi[at : at + group], lo[at : at + group]
            total += mm(h, jnp.concatenate([h, l], axis=0), NT)
        acc_sends[...] = total
        return carry

    lax.fori_loop(0, steps, body, 0)
    cross = acc_frames[:, frames:]
    body, tail = pack(acc_frames[:, :frames] + (cross + cross.T))
    cross = acc_sends[:, group:]
    pair = acc_sends[:, :group] + (cross + cross.T)
    same = iota(pair.shape, 0) // sends == iota(pair.shape, 1) // sends
    pair = jnp.where(same, pair, 0.0)
    folded = pair[:sends]
    for at in range(sends, group, sends):
        folded = folded + pair[at : at + sends]
    half = sends // 2
    pick = (iota((group, LANES), 0) % sends == iota((group, LANES), 1)).astype(F32)
    small = mmf(folded, pick, NN)
    small = small[:half] + pltpu.roll(small[half:], sends, 1)
    side = side_ref[0]
    for ref, at in ((mine_ref, side), (other_ref, 1 - side)):
        left = at == 0
        ref[: body.shape[0]] = jnp.where(left, body[:, :LANES], body[:, LANES:])
        ref[body.shape[0] :] = jnp.where(left, tail[:, :LANES] + small, tail[:, LANES:])


def signal_grams(flat, sends, side, col):
    rows, frames = flat.shape
    block = min(rows, 1024)
    shape = (frames // 2 + SUB, LANES)
    return pl.pallas_call(
        functools.partial(gram_kernel, sends, block, 3),
        in_specs=[pl.BlockSpec(memory_space=pltpu.HBM)] + [pl.BlockSpec(memory_space=pltpu.SMEM)] * 2,
        out_specs=[VSPEC] * 3,
        out_shape=[VMEM(flat.shape, F32)] + [jax.ShapeDtypeStruct(shape, F32)] * 2,
        scratch_shapes=[
            VMEM((frames, 2 * frames), F32),
            VMEM((LANES, 2 * LANES), F32),
            pltpu.SemaphoreType.DMA((rows // block,)),
        ],
        compiler_params=params(),
        name="signal_grams",
    )(pltpu.with_memory_space_constraint(flat, pltpu.HBM), side, col)


def sweep(inner, image):
    count = inner.shape[0]
    blocks = count // SUB
    tiles = image.shape[1] // LANES
    a = [inner[SUB * i : SUB * (i + 1)] for i in range(blocks)]
    z = [
        [image[SUB * i : SUB * (i + 1), LANES * t : LANES * (t + 1)] for t in range(tiles)]
        for i in range(blocks)
    ]
    row = iota((SUB, LANES), 0)
    done = []
    for j in range(blocks):
        cols = [
            {i: jnp.broadcast_to(a[i][:, SUB * j + k : SUB * j + k + 1], (SUB, LANES)) for i in range(j, blocks)}
            for k in range(SUB)
        ]
        scale = jnp.zeros((SUB, LANES), F32)
        for k in range(SUB):
            pivot = jnp.broadcast_to(cols[k][j][k : k + 1], (SUB, LANES))
            inverse = 1.0 / pivot
            scale = jnp.where(row == k, lax.rsqrt(pivot), scale)
            a_row = jnp.broadcast_to(a[j][k : k + 1], (SUB, LANES)) * inverse
            z_row = [jnp.broadcast_to(t[k : k + 1], (SUB, LANES)) * inverse for t in z[j]]
            c_row = {
                q: jnp.broadcast_to(cols[q][j][k : k + 1], (SUB, LANES)) * inverse for q in range(k + 1, SUB)
            }
            for i in range(j, blocks):
                by = cols[k][i]
                if i == j:
                    by = jnp.where(row > k, by, 0.0)
                for q in range(k + 1, SUB):
                    cols[q][i] = cols[q][i] - by * c_row[q]
                if j + 1 < blocks:
                    a[i] = a[i] - by * a_row
                z[i] = [t - by * r for t, r in zip(z[i], z_row)]
        done.append([t * scale for t in z[j]])
    lines = [jnp.concatenate(d, axis=1) if tiles > 1 else d[0] for d in done]
    return jnp.concatenate(lines, axis=0) if blocks > 1 else lines[0]


def orthonormal(gram, start):
    def body(_, basis):
        image = mmf(basis, gram, NN)
        count = image.shape[0]
        padded = jnp.concatenate([image, jnp.zeros((LANES - count, image.shape[1]), F32)], axis=0)
        return sweep(mmf(image, padded, NT), image)

    return lax.fori_loop(0, ITERS, body, start)


def small_bases_kernel(
    kmax, cols, sends, mine_ref, other_ref, side_ref, sf_ref, ss_ref, rf_ref, rs_ref, frames_ref, spread_ref
):
    h = mine_ref.shape[0] - SUB
    left = side_ref[0] == 0
    mine, other = mine_ref[...], other_ref[...]
    first, last = jnp.where(left, mine, other), jnp.where(left, other, mine)
    gram_f = unpack(jnp.concatenate([first[:h], last[:h]], axis=1), jnp.concatenate([first[h:], last[h:]], axis=1))
    small = first[h:]
    lane = iota(small.shape, 1)
    gram_s = jnp.concatenate(
        [
            jnp.where(lane < sends, small, 0.0),
            jnp.where(lane < sends, pltpu.roll(small, LANES - sends, 1), 0.0),
            jnp.zeros((LANES - sends, LANES), F32),
        ],
        axis=0,
    )

    def body(_, bases):
        images = [mmf(basis, gram, NN) for basis, gram in zip(bases, (gram_f, gram_s))]
        inners = [
            mmf(i, jnp.concatenate([i, jnp.zeros((LANES - i.shape[0], i.shape[1]), F32)], axis=0), NT) for i in images
        ]
        return tuple(sweep(n, i) for n, i in zip(inners, images))

    basis_f, basis_s = lax.fori_loop(0, ITERS, body, (sf_ref[...], ss_ref[...]))
    frames_ref[...] = jnp.where(iota(basis_f.shape, 0) < rf_ref[0], basis_f, 0.0)
    basis_s = jnp.where(iota(basis_s.shape, 0) < rs_ref[0], basis_s, 0.0)
    pick = (iota((kmax, kmax * cols), 0) == iota((kmax, kmax * cols), 1) // cols).astype(F32)
    spread_ref[...] = mmf(basis_s, pick, TN)[:sends]


def small_bases(mine, other, side, start_frames, start_sends, rank_frames, rank_sends, cols):
    frames, tmax = start_frames.shape
    sends, kmax = start_sends.shape
    padded = jnp.pad(start_sends.T, ((0, 0), (0, LANES - sends)))
    smem = pl.BlockSpec(memory_space=pltpu.SMEM)
    return pl.pallas_call(
        functools.partial(small_bases_kernel, kmax, cols, sends),
        in_specs=[VSPEC, VSPEC, smem, VSPEC, VSPEC, smem, smem],
        out_specs=[VSPEC, VSPEC],
        out_shape=[jax.ShapeDtypeStruct((tmax, frames), F32), jax.ShapeDtypeStruct((sends, kmax * cols), F32)],
        compiler_params=params(),
        name="small_bases",
    )(mine, other, side, start_frames.T, padded, rank_frames, rank_sends)


def mixing(spread, cols):
    sends, wide = spread.shape
    tall = jnp.broadcast_to(spread[None], (cols, sends, wide)).reshape(cols * sends, wide)
    same = iota(tall.shape, 0) // sends == iota(tall.shape, 1) % cols
    return jnp.where(same, tall, 0.0)


def core_kernel(lanes, cols, per, x_ref, basis_ref, spread_ref, out_ref, held, mix_ref):
    tmax = basis_ref.shape[0]
    mix_ref[0], mix_ref[1] = split2(mixing(spread_ref[...], cols))
    bh, bl = split2(basis_ref[...])
    base = jnp.concatenate([bh, bl], axis=0)
    span = mix_ref.shape[1]

    def body(step, carry):
        his, los = [], []
        for q in range(per):
            at = pl.multiple_of((step * per + q) * span, span)
            xh, xl = split2(x_ref[pl.ds(at, span), :])
            both = mm(base, xh, NT)
            h, l = split2(both[:tmax] + (both[tmax:] + mm(bh, xl, NT)))
            his.append(h)
            los.append(l)
        rows = per * tmax
        stack = jnp.concatenate(his + los, axis=0)
        both = mm(stack, mix_ref[0], NN)
        c = both[:rows] + (both[rows:] + mm(stack[:rows], mix_ref[1], NN))
        for q in range(per):
            for h in range(c.shape[1] // lanes):
                held[step * per + q, h * tmax : (h + 1) * tmax] = c[
                    q * tmax : (q + 1) * tmax, h * lanes : (h + 1) * lanes
                ]
        return carry

    lax.fori_loop(0, held.shape[0] // per, body, 0)
    for r in range(held.shape[0]):
        out_ref[:, r, :] = held[r]


def project(flat, basis, spread, rows_dev, cols, lanes):
    tmax = basis.shape[0]
    sends, wide = spread.shape
    span = cols * sends
    per = 2 if rows_dev % 2 == 0 else 1
    high = wide * tmax // lanes
    return pl.pallas_call(
        functools.partial(core_kernel, lanes, cols, per),
        in_specs=[VSPEC] * 3,
        out_specs=VSPEC,
        out_shape=VMEM((high, rows_dev, lanes), F32),
        scratch_shapes=[VMEM((rows_dev, high, lanes), F32), VMEM((2, span, wide), BF16)],
        compiler_params=params(),
        name="project",
    )(flat, basis, spread)


def block_of(ref, j, g):
    part = ref[:, j, g]
    return part.reshape(part.shape[0] * part.shape[1], part.shape[2])


def row_gram_kernel(m_ref, col_ref, out_ref, *piece_refs):
    sections = m_ref.shape[1]
    for by, piece_ref in enumerate(piece_refs):
        to = lax.rem(col_ref[0] + by, sections)
        for i in range(m_ref.shape[0]):
            for g in range(m_ref.shape[2]):
                piece_ref[i, g] = m_ref[i, to, g]
    total = None
    cross = None
    for j in range(m_ref.shape[1]):
        for g in range(m_ref.shape[2]):
            h, l = split2(block_of(m_ref, j, g))
            hh, hl = mm(h, h, NT), mm(h, l, NT)
            total = hh if total is None else total + hh
            cross = hl if cross is None else cross + hl
    put(out_ref, total + (cross + cross.T))


def put(ref, square):
    body, tail = pack(square)
    ref[: body.shape[0]] = body
    ref[body.shape[0] :] = tail


def get(ref):
    h = ref.shape[0] - SUB
    return unpack(ref[:h], ref[h:])


def row_gram(m, col):
    rows = m.shape[0] * m.shape[3]
    piece = jax.ShapeDtypeStruct((m.shape[0],) + m.shape[2:], F32)
    sections = m.shape[1]
    return pl.pallas_call(
        row_gram_kernel,
        in_specs=[VSPEC, pl.BlockSpec(memory_space=pltpu.SMEM)],
        out_specs=[VSPEC] * (1 + sections),
        out_shape=[jax.ShapeDtypeStruct((rows // 2 + SUB, rows), F32)] + [piece] * sections,
        compiler_params=params(),
        name="row_gram",
    )(m, col)


def second_kernel(cols, gram_ref, start_ref, col_ref, *refs):
    piece_refs = refs[:-3]
    basis_ref, second_ref, out_ref = refs[-3:]
    basis = orthonormal(get(gram_ref), start_ref[...])
    basis_ref[...] = basis
    uh, ul = split2(basis)
    twice = jnp.concatenate([uh, uh], axis=1)
    sections = len(piece_refs)
    low = piece_refs[0].shape[3] // cols
    total = None
    cross = None
    contract = (((0,), (1,)), ((), ()))
    for g in range(piece_refs[0].shape[1]):
        for by, piece_ref in enumerate(piece_refs):
            at = pl.multiple_of(lax.rem(col_ref[0] + (sections - by), sections) * cols, cols)
            part = piece_ref[:, g]
            h, l = split2(part.reshape(part.shape[0] * part.shape[1], part.shape[2]))
            t = mm(jnp.concatenate([h, l], axis=0), twice, contract) + mm(h, ul, contract)
            for e in range(low):
                second_ref[g * low + e, pl.ds(at, cols)] = t[e * cols : (e + 1) * cols]
        for e in range(low):
            h, l = split2(second_ref[g * low + e])
            hh, hl = mm(h, h, NT), mm(h, l, NT)
            total = hh if total is None else total + hh
            cross = hl if cross is None else cross + hl
    put(out_ref, total + (cross + cross.T))


def second_stage(gram, start, col, pieces, cols):
    rows, kept = start.shape
    sections, groups, lanes = len(pieces), pieces[0].shape[1], pieces[0].shape[3]
    low = lanes // cols
    wide = sections * cols
    return pl.pallas_call(
        functools.partial(second_kernel, cols),
        in_specs=[VSPEC, VSPEC, pl.BlockSpec(memory_space=pltpu.SMEM)] + [VSPEC] * sections,
        out_specs=[VSPEC] * 3,
        out_shape=[
            jax.ShapeDtypeStruct((kept, rows), F32),
            jax.ShapeDtypeStruct((groups * low, wide, kept), F32),
            jax.ShapeDtypeStruct((wide // 2 + SUB, wide), F32),
        ],
        compiler_params=params(),
        name="second_stage",
    )(gram, start.T, col, *pieces)


def third_kernel(cols, gram_ref, start_ref, basis_ref, second_ref, out_ref):
    basis_c = orthonormal(get(gram_ref), start_ref[...])
    ph, pl_ = split2(mmf(basis_c, basis_c, TN))
    twice = jnp.concatenate([ph, ph], axis=1)
    rows_t = split2(basis_ref[...].T)
    sections = out_ref.shape[1]
    low = out_ref.shape[4] // cols
    for g in range(out_ref.shape[2]):
        kept = []
        for e in range(low):
            h, l = split2(second_ref[g * low + e])
            kept.append(split2(mm(twice, jnp.concatenate([h, l], axis=0), NN) + mm(pl_, h, NN)))
        for j in range(sections):
            part = [
                jnp.concatenate([k[w][j * cols : (j + 1) * cols] for k in kept], axis=0) for w in range(2)
            ]
            t = mm2(rows_t, part, NT)
            out_ref[:, j, g] = t.reshape(out_ref.shape[0], out_ref.shape[3], out_ref.shape[4])


def third_stage(gram, start, basis, second, shape, cols):
    return pl.pallas_call(
        functools.partial(third_kernel, cols),
        in_specs=[VSPEC] * 4,
        out_specs=VSPEC,
        out_shape=VMEM(shape, F32),
        compiler_params=params(),
        name="third_stage",
    )(gram, start.T, basis, second)


def expand_kernel(cols, per, x_ref, t_ref, basis_ref, spread_ref, out_ref, held, mix_ref, base_ref):
    step = pl.program_id(0)
    tmax = basis_ref.shape[0]

    @pl.when(step == 0)
    def _():
        hi, lo = split2(mixing(spread_ref[...], cols))
        mix_ref[0], mix_ref[1] = hi.T, lo.T
        hi, lo = split2(basis_ref[...])
        for q, part in enumerate((hi, lo, hi)):
            base_ref[q * tmax : (q + 1) * tmax] = part
        for r in range(held.shape[0]):
            held[r] = t_ref[:, r, :]

    span = mix_ref.shape[2]
    tiles = []
    for q in range(per):
        t = held[step * per + q]
        tiles.append(jnp.concatenate([t[h * tmax : (h + 1) * tmax] for h in range(t.shape[0] // tmax)], axis=1))
    hi, lo = split2(jnp.concatenate(tiles, axis=0))
    rows = per * tmax
    both = mm(jnp.concatenate([hi, lo], axis=0), mix_ref[0], NN)
    zh, zl = split2(both[:rows] + (both[rows:] + mm(hi, mix_ref[1], NN)))
    for q in range(per):
        h, l = zh[q * tmax : (q + 1) * tmax], zl[q * tmax : (q + 1) * tmax]
        tissue = mm(jnp.concatenate([h, h, l], axis=0), base_ref[...], TN)
        at = pl.multiple_of((step * per + q) * span, span)
        out_ref[q * span : (q + 1) * span] = x_ref[pl.ds(at, span), :] - tissue


def expand(flat, t, basis, spread, cols):
    rows, frames = flat.shape
    tmax = basis.shape[0]
    sends, wide = spread.shape
    high, rows_dev, lanes = t.shape
    span = cols * sends
    per = 2 if rows_dev % 2 == 0 else 1
    return pl.pallas_call(
        functools.partial(expand_kernel, cols, per),
        grid=(rows // (span * per),),
        in_specs=[VSPEC] * 4,
        out_specs=pl.BlockSpec((span * per, frames), lambda i: (i, 0)),
        out_shape=jax.ShapeDtypeStruct(flat.shape, F32),
        scratch_shapes=[
            VMEM((rows_dev, high, lanes), F32),
            VMEM((2, wide, span), BF16),
            VMEM((3 * tmax, frames), BF16),
        ],
        compiler_params=params(),
        name="expand",
    )(flat, t, basis, spread)


def shifted(x, axis, by, size):
    return lax.ppermute(x, axis, [(i, (i + by) % size) for i in range(size)])


def exchange_sum(x, axis, size, stride=1):
    total = x
    for by in range(stride, size, stride):
        total = total + shifted(x, axis, by, size)
    return total


def sum_all(x, rows, cols):
    x = exchange_sum(x, "col", cols)
    if rows % 2 or rows == 2:
        return exchange_sum(x, "row", rows)
    x = exchange_sum(x, "row", rows, 2)
    return x + lax.ppermute(x, "row", [(i, i ^ 1) for i in range(rows)])


def sum_halves(mine, other, rows, cols):
    pairs = [(i, i ^ 1) for i in range(rows)]
    mine = mine + lax.ppermute(other, "row", pairs)
    mine = exchange_sum(mine, "row", rows, 2)
    mine = exchange_sum(mine, "col", cols)
    return mine, lax.ppermute(mine, "row", pairs)


def local(rows, cols, signal, start_frames, start_sends, start_rows, start_cols, rank_frames, rank_sends):
    rows_dev, cols_dev, sends, frames = signal.shape
    kmax, tmax = start_sends.shape[1], start_frames.shape[1]
    devices = rows * cols
    flat = signal.reshape(-1, frames)
    side = (lax.axis_index("row") % 2).astype(jnp.int32).reshape(1)

    col = lax.axis_index("col").astype(jnp.int32).reshape(1)

    near, mine, other = signal_grams(flat, sends, side, col)
    mine, other = sum_halves(mine, other, rows, cols)
    basis, spread = small_bases(
        mine, other, side, start_frames, start_sends, rank_frames, rank_sends, cols_dev
    )

    low = min(LANES // cols_dev, kmax * tmax // devices, kmax)
    lanes = low * cols_dev
    near = in_vmem(near)
    core = project(near, basis, spread, rows_dev, cols_dev, lanes)
    groups = core.shape[0] // devices
    m = lax.all_to_all(core.reshape(rows, cols, groups, rows_dev, lanes), "row", 0, 0)

    gram_rows, *pieces = row_gram(m, col)
    pieces = [pieces[0]] + [shifted(piece, "col", by, cols) for by, piece in enumerate(pieces) if by]
    gram_rows = sum_all(gram_rows, rows, cols)
    basis_rows, second, gram_cols = second_stage(gram_rows, start_rows, col, pieces, cols_dev)
    gram_cols = sum_all(gram_cols, rows, cols)
    t = third_stage(gram_cols, start_cols, basis_rows, second, m.shape, cols_dev)

    t = t.reshape(devices, groups, rows_dev, lanes)
    t = lax.all_to_all(t, ("row", "col"), 0, 0).reshape(devices * groups, rows_dev, lanes)
    return expand(near, t, basis, spread, cols_dev).reshape(signal.shape)


def solution(mesh):
    rows, cols = mesh.shape["row"], mesh.shape["col"]
    return jax.shard_map(
        functools.partial(local, rows, cols),
        mesh=mesh,
        in_specs=(P("row", "col", None, None), P(), P(), P(), P(), P(), P()),
        out_specs=P("row", "col", None, None),
        check_vma=False,
    )
```

```python
import functools

import jax
import jax.numpy as jnp
from jax import lax
from jax.experimental import pallas as pl
from jax.experimental.pallas import tpu as pltpu
from jax.sharding import PartitionSpec as P


ITERS = 2
LANES = 128
SUB = 8
HIGH = lax.Precision.HIGHEST
F32 = jnp.float32
BF16 = jnp.bfloat16
VMEM = pltpu.VMEM


NN = (((1,), (0,)), ((), ()))
NT = (((1,), (1,)), ((), ()))
TN = (((0,), (0,)), ((), ()))


def mm(a, b, dims):
    return lax.dot_general(a, b, dims, preferred_element_type=F32)


def mmf(a, b, dims):
    return lax.dot_general(a, b, dims, precision=HIGH, preferred_element_type=F32)


def split2(x):
    hi = x.astype(BF16)
    return hi, (x - hi.astype(F32)).astype(BF16)


def iota(shape, dim):
    return lax.broadcasted_iota(jnp.int32, shape, dim)


def params(mib=24):
    return pltpu.CompilerParams(vmem_limit_bytes=mib * 2**20)


VSPEC = pl.BlockSpec(memory_space=VMEM)


def in_vmem(x):
    return pltpu.with_memory_space_constraint(x, VMEM)


def mm2(a, b, dims_last):
    (ah, al), (bh, bl) = a, b
    return mm(ah, bh, dims_last) + (mm(ah, bl, dims_last) + mm(al, bh, dims_last))


def pack(square):
    n = square.shape[0]
    h = n // 2
    top, low = square[:h], square[h:]
    row, lane = iota((h, n), 0), iota((h, n), 1)
    turned = pltpu.roll(low, h, 1)
    body = jnp.where(lane < row, turned, top)
    diag = jnp.sum(jnp.where(lane == row + h, low, 0.0), axis=0, keepdims=True)
    tail = jnp.where(iota((SUB, n), 0) == 0, jnp.broadcast_to(diag, (SUB, n)), 0.0)
    return body, tail


def unpack(body, tail):
    h, n = body.shape
    row, lane = iota((h, n), 0), iota((h, n), 1)
    flip = body.T
    first, last = flip[:h], flip[h:]
    if h % LANES:
        zeros = jnp.zeros((h, n - h), F32)
        first, last = jnp.concatenate([first, zeros], axis=1), jnp.concatenate([last, zeros], axis=1)
    else:
        first, last = jnp.concatenate([first, first], axis=1), jnp.concatenate([last, last], axis=1)
    top = jnp.where(lane < row, first, body)
    corner = pltpu.roll(jnp.where(lane < row, body, first), h, 1)
    corner = jnp.where(lane == row + h, jnp.broadcast_to(tail[:1], (h, n)), corner)
    return jnp.concatenate([top, jnp.where(lane < h, last, corner)], axis=0)


def gram_kernel(sends, block, x_ref, side_ref, col_ref, near_ref, mine_ref, other_ref, acc_frames, acc_sends, sems):
    frames = x_ref.shape[1]
    group = acc_sends.shape[0]
    rows = x_ref.shape[0]
    piece = rows // sems.shape[0]

    def copy(step):
        at = pl.ds(pl.multiple_of(step * piece, piece), piece)
        return pltpu.make_async_copy(x_ref.at[at, :], near_ref.at[at, :], sems.at[step])

    for step in range(rows // piece):
        copy(step).start()
    acc_frames[...] = jnp.zeros_like(acc_frames)
    acc_sends[...] = jnp.zeros_like(acc_sends)

    def body(step, carry):
        for q in range(block // piece):
            copy(step * (block // piece) + q).wait()
        hi, lo = split2(near_ref[pl.ds(pl.multiple_of(step * block, block), block), :])
        acc_frames[...] += mm(hi, jnp.concatenate([hi, lo], axis=1), TN)
        total = acc_sends[...]
        for at in range(0, block, group):
            h, l = hi[at : at + group], lo[at : at + group]
            total += mm(h, jnp.concatenate([h, l], axis=0), NT)
        acc_sends[...] = total
        return carry

    lax.fori_loop(0, rows // block, body, 0)
    cross = acc_frames[:, frames:]
    body, tail = pack(acc_frames[:, :frames] + (cross + cross.T))
    cross = acc_sends[:, group:]
    pair = acc_sends[:, :group] + (cross + cross.T)
    same = iota(pair.shape, 0) // sends == iota(pair.shape, 1) // sends
    pair = jnp.where(same, pair, 0.0)
    folded = pair[:sends]
    for at in range(sends, group, sends):
        folded = folded + pair[at : at + sends]
    half = sends // 2
    pick = (iota((group, LANES), 0) % sends == iota((group, LANES), 1)).astype(F32)
    small = mmf(folded, pick, NN)
    small = small[:half] + pltpu.roll(small[half:], sends, 1)
    side = side_ref[0]
    for ref, at in ((mine_ref, side), (other_ref, 1 - side)):
        left = at == 0
        ref[: body.shape[0]] = jnp.where(left, body[:, :LANES], body[:, LANES:])
        ref[body.shape[0] :] = jnp.where(left, tail[:, :LANES] + small, tail[:, LANES:])


def signal_grams(flat, sends, side, col):
    rows, frames = flat.shape
    block = min(rows, 2048)
    piece = min(rows, 512)
    shape = (frames // 2 + SUB, LANES)
    return pl.pallas_call(
        functools.partial(gram_kernel, sends, block),
        in_specs=[pl.BlockSpec(memory_space=pltpu.HBM)] + [pl.BlockSpec(memory_space=pltpu.SMEM)] * 2,
        out_specs=[VSPEC] * 3,
        out_shape=[VMEM(flat.shape, F32)] + [jax.ShapeDtypeStruct(shape, F32)] * 2,
        scratch_shapes=[
            VMEM((frames, 2 * frames), F32),
            VMEM((LANES, 2 * LANES), F32),
            pltpu.SemaphoreType.DMA((rows // piece,)),
        ],
        compiler_params=params(),
        name="signal_grams",
    )(pltpu.with_memory_space_constraint(flat, pltpu.HBM), side, col)


def sweep(inner, image):
    count = inner.shape[0]
    blocks = count // SUB
    tiles = image.shape[1] // LANES
    a = [inner[SUB * i : SUB * (i + 1)] for i in range(blocks)]
    z = [
        [image[SUB * i : SUB * (i + 1), LANES * t : LANES * (t + 1)] for t in range(tiles)]
        for i in range(blocks)
    ]
    row = iota((SUB, LANES), 0)
    done = []
    for j in range(blocks):
        cols = [
            {i: jnp.broadcast_to(a[i][:, SUB * j + k : SUB * j + k + 1], (SUB, LANES)) for i in range(j, blocks)}
            for k in range(SUB)
        ]
        scale = jnp.zeros((SUB, LANES), F32)
        for k in range(SUB):
            pivot = jnp.broadcast_to(cols[k][j][k : k + 1], (SUB, LANES))
            inverse = 1.0 / pivot
            scale = jnp.where(row == k, lax.rsqrt(pivot), scale)
            a_row = jnp.broadcast_to(a[j][k : k + 1], (SUB, LANES)) * inverse
            z_row = [jnp.broadcast_to(t[k : k + 1], (SUB, LANES)) * inverse for t in z[j]]
            c_row = {
                q: jnp.broadcast_to(cols[q][j][k : k + 1], (SUB, LANES)) * inverse for q in range(k + 1, SUB)
            }
            for i in range(j, blocks):
                by = cols[k][i]
                if i == j:
                    by = jnp.where(row > k, by, 0.0)
                for q in range(k + 1, SUB):
                    cols[q][i] = cols[q][i] - by * c_row[q]
                if j + 1 < blocks:
                    a[i] = a[i] - by * a_row
                z[i] = [t - by * r for t, r in zip(z[i], z_row)]
        done.append([t * scale for t in z[j]])
    lines = [jnp.concatenate(d, axis=1) if tiles > 1 else d[0] for d in done]
    return jnp.concatenate(lines, axis=0) if blocks > 1 else lines[0]


def orthonormal(gram, start):
    def body(_, basis):
        image = mmf(basis, gram, NN)
        count = image.shape[0]
        padded = jnp.concatenate([image, jnp.zeros((LANES - count, image.shape[1]), F32)], axis=0)
        return sweep(mmf(image, padded, NT), image)

    return lax.fori_loop(0, ITERS, body, start)


def small_bases_kernel(
    kmax, cols, sends, mine_ref, other_ref, side_ref, sf_ref, ss_ref, rf_ref, rs_ref, frames_ref, spread_ref
):
    h = mine_ref.shape[0] - SUB
    left = side_ref[0] == 0
    mine, other = mine_ref[...], other_ref[...]
    first, last = jnp.where(left, mine, other), jnp.where(left, other, mine)
    gram_f = unpack(jnp.concatenate([first[:h], last[:h]], axis=1), jnp.concatenate([first[h:], last[h:]], axis=1))
    small = first[h:]
    lane = iota(small.shape, 1)
    gram_s = jnp.concatenate(
        [
            jnp.where(lane < sends, small, 0.0),
            jnp.where(lane < sends, pltpu.roll(small, LANES - sends, 1), 0.0),
            jnp.zeros((LANES - sends, LANES), F32),
        ],
        axis=0,
    )

    def body(_, bases):
        images = [mmf(basis, gram, NN) for basis, gram in zip(bases, (gram_f, gram_s))]
        inners = [
            mmf(i, jnp.concatenate([i, jnp.zeros((LANES - i.shape[0], i.shape[1]), F32)], axis=0), NT) for i in images
        ]
        return tuple(sweep(n, i) for n, i in zip(inners, images))

    basis_f, basis_s = lax.fori_loop(0, ITERS, body, (sf_ref[...], ss_ref[...]))
    frames_ref[...] = jnp.where(iota(basis_f.shape, 0) < rf_ref[0], basis_f, 0.0)
    basis_s = jnp.where(iota(basis_s.shape, 0) < rs_ref[0], basis_s, 0.0)
    pick = (iota((kmax, kmax * cols), 0) == iota((kmax, kmax * cols), 1) // cols).astype(F32)
    spread_ref[...] = mmf(basis_s, pick, TN)[:sends]


def small_bases(mine, other, side, start_frames, start_sends, rank_frames, rank_sends, cols):
    frames, tmax = start_frames.shape
    sends, kmax = start_sends.shape
    padded = jnp.pad(start_sends.T, ((0, 0), (0, LANES - sends)))
    smem = pl.BlockSpec(memory_space=pltpu.SMEM)
    return pl.pallas_call(
        functools.partial(small_bases_kernel, kmax, cols, sends),
        in_specs=[VSPEC, VSPEC, smem, VSPEC, VSPEC, smem, smem],
        out_specs=[VSPEC, VSPEC],
        out_shape=[jax.ShapeDtypeStruct((tmax, frames), F32), jax.ShapeDtypeStruct((sends, kmax * cols), F32)],
        compiler_params=params(),
        name="small_bases",
    )(mine, other, side, start_frames.T, padded, rank_frames, rank_sends)


def mixing(spread, cols):
    sends, wide = spread.shape
    tall = jnp.broadcast_to(spread[None], (cols, sends, wide)).reshape(cols * sends, wide)
    same = iota(tall.shape, 0) // sends == iota(tall.shape, 1) % cols
    return jnp.where(same, tall, 0.0)


def core_kernel(lanes, cols, per, x_ref, basis_ref, spread_ref, out_ref, held, mix_ref):
    tmax = basis_ref.shape[0]
    mix_ref[0], mix_ref[1] = split2(mixing(spread_ref[...], cols))
    bh, bl = split2(basis_ref[...])
    base = jnp.concatenate([bh, bl], axis=0)
    span = mix_ref.shape[1]

    def body(step, carry):
        his, los = [], []
        for q in range(per):
            at = pl.multiple_of((step * per + q) * span, span)
            xh, xl = split2(x_ref[pl.ds(at, span), :])
            both = mm(base, xh, NT)
            h, l = split2(both[:tmax] + (both[tmax:] + mm(bh, xl, NT)))
            his.append(h)
            los.append(l)
        rows = per * tmax
        stack = jnp.concatenate(his + los, axis=0)
        both = mm(stack, mix_ref[0], NN)
        c = both[:rows] + (both[rows:] + mm(stack[:rows], mix_ref[1], NN))
        for q in range(per):
            for h in range(c.shape[1] // lanes):
                held[step * per + q, h * tmax : (h + 1) * tmax] = c[
                    q * tmax : (q + 1) * tmax, h * lanes : (h + 1) * lanes
                ]
        return carry

    lax.fori_loop(0, held.shape[0] // per, body, 0)
    for r in range(held.shape[0]):
        out_ref[:, r, :] = held[r]


def project(flat, basis, spread, rows_dev, cols, lanes):
    tmax = basis.shape[0]
    sends, wide = spread.shape
    span = cols * sends
    per = 2 if rows_dev % 2 == 0 else 1
    high = wide * tmax // lanes
    return pl.pallas_call(
        functools.partial(core_kernel, lanes, cols, per),
        in_specs=[VSPEC] * 3,
        out_specs=VSPEC,
        out_shape=VMEM((high, rows_dev, lanes), F32),
        scratch_shapes=[VMEM((rows_dev, high, lanes), F32), VMEM((2, span, wide), BF16)],
        compiler_params=params(),
        name="project",
    )(flat, basis, spread)


def block_of(ref, j, g):
    part = ref[:, j, g]
    return part.reshape(part.shape[0] * part.shape[1], part.shape[2])


def row_gram_kernel(m_ref, col_ref, out_ref, *piece_refs):
    sections = m_ref.shape[1]
    for by, piece_ref in enumerate(piece_refs):
        to = lax.rem(col_ref[0] + by, sections)
        for i in range(m_ref.shape[0]):
            for g in range(m_ref.shape[2]):
                piece_ref[i, g] = m_ref[i, to, g]
    total = None
    cross = None
    for j in range(m_ref.shape[1]):
        for g in range(m_ref.shape[2]):
            h, l = split2(block_of(m_ref, j, g))
            hh, hl = mm(h, h, NT), mm(h, l, NT)
            total = hh if total is None else total + hh
            cross = hl if cross is None else cross + hl
    put(out_ref, total + (cross + cross.T))


def put(ref, square):
    body, tail = pack(square)
    ref[: body.shape[0]] = body
    ref[body.shape[0] :] = tail


def get(ref):
    h = ref.shape[0] - SUB
    return unpack(ref[:h], ref[h:])


def row_gram(m, col):
    rows = m.shape[0] * m.shape[3]
    piece = jax.ShapeDtypeStruct((m.shape[0],) + m.shape[2:], F32)
    sections = m.shape[1]
    return pl.pallas_call(
        row_gram_kernel,
        in_specs=[VSPEC, pl.BlockSpec(memory_space=pltpu.SMEM)],
        out_specs=[VSPEC] * (1 + sections),
        out_shape=[jax.ShapeDtypeStruct((rows // 2 + SUB, rows), F32)] + [piece] * sections,
        compiler_params=params(),
        name="row_gram",
    )(m, col)


def second_kernel(cols, gram_ref, start_ref, col_ref, *refs):
    piece_refs = refs[:-3]
    basis_ref, second_ref, out_ref = refs[-3:]
    basis = orthonormal(get(gram_ref), start_ref[...])
    basis_ref[...] = basis
    uh, ul = split2(basis)
    twice = jnp.concatenate([uh, uh], axis=1)
    sections = len(piece_refs)
    low = piece_refs[0].shape[3] // cols
    total = None
    cross = None
    contract = (((0,), (1,)), ((), ()))
    for g in range(piece_refs[0].shape[1]):
        for by, piece_ref in enumerate(piece_refs):
            at = pl.multiple_of(lax.rem(col_ref[0] + (sections - by), sections) * cols, cols)
            part = piece_ref[:, g]
            h, l = split2(part.reshape(part.shape[0] * part.shape[1], part.shape[2]))
            t = mm(jnp.concatenate([h, l], axis=0), twice, contract) + mm(h, ul, contract)
            for e in range(low):
                second_ref[g * low + e, pl.ds(at, cols)] = t[e * cols : (e + 1) * cols]
        for e in range(low):
            h, l = split2(second_ref[g * low + e])
            hh, hl = mm(h, h, NT), mm(h, l, NT)
            total = hh if total is None else total + hh
            cross = hl if cross is None else cross + hl
    put(out_ref, total + (cross + cross.T))


def second_stage(gram, start, col, pieces, cols):
    rows, kept = start.shape
    sections, groups, lanes = len(pieces), pieces[0].shape[1], pieces[0].shape[3]
    low = lanes // cols
    wide = sections * cols
    return pl.pallas_call(
        functools.partial(second_kernel, cols),
        in_specs=[VSPEC, VSPEC, pl.BlockSpec(memory_space=pltpu.SMEM)] + [VSPEC] * sections,
        out_specs=[VSPEC] * 3,
        out_shape=[
            jax.ShapeDtypeStruct((kept, rows), F32),
            jax.ShapeDtypeStruct((groups * low, wide, kept), F32),
            jax.ShapeDtypeStruct((wide // 2 + SUB, wide), F32),
        ],
        compiler_params=params(),
        name="second_stage",
    )(gram, start.T, col, *pieces)


def third_kernel(cols, gram_ref, start_ref, basis_ref, second_ref, out_ref):
    basis_c = orthonormal(get(gram_ref), start_ref[...])
    ph, pl_ = split2(mmf(basis_c, basis_c, TN))
    twice = jnp.concatenate([ph, ph], axis=1)
    rows_t = split2(basis_ref[...].T)
    sections = out_ref.shape[1]
    low = out_ref.shape[4] // cols
    for g in range(out_ref.shape[2]):
        kept = []
        for e in range(low):
            h, l = split2(second_ref[g * low + e])
            kept.append(split2(mm(twice, jnp.concatenate([h, l], axis=0), NN) + mm(pl_, h, NN)))
        for j in range(sections):
            part = [
                jnp.concatenate([k[w][j * cols : (j + 1) * cols] for k in kept], axis=0) for w in range(2)
            ]
            t = mm2(rows_t, part, NT)
            out_ref[:, j, g] = t.reshape(out_ref.shape[0], out_ref.shape[3], out_ref.shape[4])


def third_stage(gram, start, basis, second, shape, cols):
    return pl.pallas_call(
        functools.partial(third_kernel, cols),
        in_specs=[VSPEC] * 4,
        out_specs=VSPEC,
        out_shape=VMEM(shape, F32),
        compiler_params=params(),
        name="third_stage",
    )(gram, start.T, basis, second)


def expand_kernel(cols, per, x_ref, t_ref, basis_ref, spread_ref, out_ref, stage, held, mix_ref, base_ref, sems):
    tmax = basis_ref.shape[0]
    hi, lo = split2(mixing(spread_ref[...], cols))
    mix_ref[0], mix_ref[1] = hi.T, lo.T
    hi, lo = split2(basis_ref[...])
    for q, part in enumerate((hi, lo, hi)):
        base_ref[q * tmax : (q + 1) * tmax] = part
    for r in range(held.shape[0]):
        held[r] = t_ref[:, r, :]

    span = mix_ref.shape[2]
    rows = per * tmax
    steps = held.shape[0] // per

    def copy(step):
        at = pl.ds(pl.multiple_of(step * per * span, per * span), per * span)
        return pltpu.make_async_copy(stage.at[at, :], out_ref.at[at, :], sems.at[step])

    def body(step, carry):
        @pl.when(step > 0)
        def _():
            copy(step - 1).start()

        tiles = []
        for q in range(per):
            t = held[step * per + q]
            tiles.append(jnp.concatenate([t[h * tmax : (h + 1) * tmax] for h in range(t.shape[0] // tmax)], axis=1))
        hi, lo = split2(jnp.concatenate(tiles, axis=0))
        both = mm(jnp.concatenate([hi, lo], axis=0), mix_ref[0], NN)
        zh, zl = split2(both[:rows] + (both[rows:] + mm(hi, mix_ref[1], NN)))
        for q in range(per):
            h, l = zh[q * tmax : (q + 1) * tmax], zl[q * tmax : (q + 1) * tmax]
            tissue = mm(jnp.concatenate([h, h, l], axis=0), base_ref[...], TN)
            at = pl.multiple_of((step * per + q) * span, span)
            stage[pl.ds(at, span), :] = x_ref[pl.ds(at, span), :] - tissue
        return carry

    lax.fori_loop(0, steps, body, 0)
    copy(steps - 1).start()
    for step in range(steps):
        copy(step).wait()


def expand(flat, t, basis, spread, cols):
    frames = flat.shape[1]
    tmax = basis.shape[0]
    sends, wide = spread.shape
    high, rows_dev, lanes = t.shape
    span = cols * sends
    per = 2 if rows_dev % 2 == 0 else 1
    return pl.pallas_call(
        functools.partial(expand_kernel, cols, per),
        in_specs=[VSPEC] * 4,
        out_specs=pl.BlockSpec(memory_space=pltpu.HBM),
        out_shape=jax.ShapeDtypeStruct(flat.shape, F32),
        scratch_shapes=[
            VMEM(flat.shape, F32),
            VMEM((rows_dev, high, lanes), F32),
            VMEM((2, wide, span), BF16),
            VMEM((3 * tmax, frames), BF16),
            pltpu.SemaphoreType.DMA((rows_dev // per,)),
        ],
        compiler_params=params(),
        name="expand",
    )(flat, t, basis, spread)


def shifted(x, axis, by, size):
    return lax.ppermute(x, axis, [(i, (i + by) % size) for i in range(size)])


def exchange_sum(x, axis, size, stride=1):
    total = x
    for by in range(stride, size, stride):
        total = total + shifted(x, axis, by, size)
    return total


def sum_all(x, rows, cols):
    x = exchange_sum(x, "col", cols)
    if rows % 2 or rows == 2:
        return exchange_sum(x, "row", rows)
    x = exchange_sum(x, "row", rows, 2)
    return x + lax.ppermute(x, "row", [(i, i ^ 1) for i in range(rows)])


def sum_halves(mine, other, rows, cols):
    pairs = [(i, i ^ 1) for i in range(rows)]
    mine = mine + lax.ppermute(other, "row", pairs)
    mine = exchange_sum(mine, "row", rows, 2)
    mine = exchange_sum(mine, "col", cols)
    return mine, lax.ppermute(mine, "row", pairs)


def local(rows, cols, signal, start_frames, start_sends, start_rows, start_cols, rank_frames, rank_sends):
    rows_dev, cols_dev, sends, frames = signal.shape
    kmax, tmax = start_sends.shape[1], start_frames.shape[1]
    devices = rows * cols
    flat = signal.reshape(-1, frames)
    side = (lax.axis_index("row") % 2).astype(jnp.int32).reshape(1)

    col = lax.axis_index("col").astype(jnp.int32).reshape(1)

    near, mine, other = signal_grams(flat, sends, side, col)
    mine, other = sum_halves(mine, other, rows, cols)
    basis, spread = small_bases(
        mine, other, side, start_frames, start_sends, rank_frames, rank_sends, cols_dev
    )

    low = min(LANES // cols_dev, kmax * tmax // devices, kmax)
    lanes = low * cols_dev
    near = in_vmem(near)
    core = project(near, basis, spread, rows_dev, cols_dev, lanes)
    groups = core.shape[0] // devices
    m = lax.all_to_all(core.reshape(rows, cols, groups, rows_dev, lanes), "row", 0, 0)

    gram_rows, *pieces = row_gram(m, col)
    pieces = [pieces[0]] + [shifted(piece, "col", by, cols) for by, piece in enumerate(pieces) if by]
    gram_rows = sum_all(gram_rows, rows, cols)
    basis_rows, second, gram_cols = second_stage(gram_rows, start_rows, col, pieces, cols_dev)
    gram_cols = sum_all(gram_cols, rows, cols)
    t = third_stage(gram_cols, start_cols, basis_rows, second, m.shape, cols_dev)

    t = t.reshape(devices, groups, rows_dev, lanes)
    t = lax.all_to_all(t, ("row", "col"), 0, 0).reshape(devices * groups, rows_dev, lanes)
    return expand(near, t, basis, spread, cols_dev).reshape(signal.shape)


def solution(mesh):
    rows, cols = mesh.shape["row"], mesh.shape["col"]
    return jax.shard_map(
        functools.partial(local, rows, cols),
        mesh=mesh,
        in_specs=(P("row", "col", None, None), P(), P(), P(), P(), P(), P()),
        out_specs=P("row", "col", None, None),
        check_vma=False,
    )
```

```python
import functools

import jax
import jax.numpy as jnp
from jax import lax
from jax.experimental import pallas as pl
from jax.experimental.pallas import tpu as pltpu
from jax.sharding import PartitionSpec as P


ITERS = 2
LANES = 128
SUB = 8
HIGH = lax.Precision.HIGHEST
F32 = jnp.float32
BF16 = jnp.bfloat16
VMEM = pltpu.VMEM


NN = (((1,), (0,)), ((), ()))
NT = (((1,), (1,)), ((), ()))
TN = (((0,), (0,)), ((), ()))


def mm(a, b, dims):
    return lax.dot_general(a, b, dims, preferred_element_type=F32)


def mmf(a, b, dims):
    return lax.dot_general(a, b, dims, precision=HIGH, preferred_element_type=F32)


def split2(x):
    hi = x.astype(BF16)
    return hi, (x - hi.astype(F32)).astype(BF16)


def target(i, by, size):
    return i ^ by if size & (size - 1) == 0 else (i + by) % size


def source(i, by, size):
    return i ^ by if size & (size - 1) == 0 else (i + (size - by)) % size


def iota(shape, dim):
    return lax.broadcasted_iota(jnp.int32, shape, dim)


def params(mib=24):
    return pltpu.CompilerParams(vmem_limit_bytes=mib * 2**20)


VSPEC = pl.BlockSpec(memory_space=VMEM)


def in_vmem(x):
    return pltpu.with_memory_space_constraint(x, VMEM)


def mm2(a, b, dims_last):
    (ah, al), (bh, bl) = a, b
    return mm(ah, bh, dims_last) + (mm(ah, bl, dims_last) + mm(al, bh, dims_last))


def pack(square):
    n = square.shape[0]
    h = n // 2
    top, low = square[:h], square[h:]
    row, lane = iota((h, n), 0), iota((h, n), 1)
    turned = pltpu.roll(low, h, 1)
    body = jnp.where(lane < row, turned, top)
    diag = jnp.sum(jnp.where(lane == row + h, low, 0.0), axis=0, keepdims=True)
    tail = jnp.where(iota((SUB, n), 0) == 0, jnp.broadcast_to(diag, (SUB, n)), 0.0)
    return body, tail


def unpack(body, tail):
    h, n = body.shape
    row, lane = iota((h, n), 0), iota((h, n), 1)
    flip = body.T
    first, last = flip[:h], flip[h:]
    if h % LANES:
        zeros = jnp.zeros((h, n - h), F32)
        first, last = jnp.concatenate([first, zeros], axis=1), jnp.concatenate([last, zeros], axis=1)
    else:
        first, last = jnp.concatenate([first, first], axis=1), jnp.concatenate([last, last], axis=1)
    top = jnp.where(lane < row, first, body)
    corner = pltpu.roll(jnp.where(lane < row, body, first), h, 1)
    corner = jnp.where(lane == row + h, jnp.broadcast_to(tail[:1], (h, n)), corner)
    return jnp.concatenate([top, jnp.where(lane < h, last, corner)], axis=0)


def gram_kernel(sends, block, x_ref, side_ref, col_ref, near_ref, mine_ref, other_ref, acc_frames, acc_sends, sems):
    frames = x_ref.shape[1]
    group = acc_sends.shape[0]
    rows = x_ref.shape[0]
    piece = rows // sems.shape[0]

    def copy(step):
        at = pl.ds(pl.multiple_of(step * piece, piece), piece)
        return pltpu.make_async_copy(x_ref.at[at, :], near_ref.at[at, :], sems.at[step])

    for step in range(rows // piece):
        copy(step).start()
    acc_frames[...] = jnp.zeros_like(acc_frames)
    acc_sends[...] = jnp.zeros_like(acc_sends)

    def body(step, carry):
        for q in range(block // piece):
            copy(step * (block // piece) + q).wait()
        hi, lo = split2(near_ref[pl.ds(pl.multiple_of(step * block, block), block), :])
        acc_frames[...] += mm(hi, jnp.concatenate([hi, lo], axis=1), TN)
        total = acc_sends[...]
        for at in range(0, block, group):
            h, l = hi[at : at + group], lo[at : at + group]
            total += mm(h, jnp.concatenate([h, l], axis=0), NT)
        acc_sends[...] = total
        return carry

    lax.fori_loop(0, rows // block, body, 0)
    cross = acc_frames[:, frames:]
    body, tail = pack(acc_frames[:, :frames] + (cross + cross.T))
    cross = acc_sends[:, group:]
    pair = acc_sends[:, :group] + (cross + cross.T)
    same = iota(pair.shape, 0) // sends == iota(pair.shape, 1) // sends
    pair = jnp.where(same, pair, 0.0)
    folded = pair[:sends]
    for at in range(sends, group, sends):
        folded = folded + pair[at : at + sends]
    half = sends // 2
    pick = (iota((group, LANES), 0) % sends == iota((group, LANES), 1)).astype(F32)
    small = mmf(folded, pick, NN)
    small = small[:half] + pltpu.roll(small[half:], sends, 1)
    side = side_ref[0]
    for ref, at in ((mine_ref, side), (other_ref, 1 - side)):
        left = at == 0
        ref[: body.shape[0]] = jnp.where(left, body[:, :LANES], body[:, LANES:])
        ref[body.shape[0] :] = jnp.where(left, tail[:, :LANES] + small, tail[:, LANES:])


def signal_grams(flat, sends, side, col):
    rows, frames = flat.shape
    block = min(rows, 2048)
    piece = min(rows, 512)
    shape = (frames // 2 + SUB, LANES)
    return pl.pallas_call(
        functools.partial(gram_kernel, sends, block),
        in_specs=[pl.BlockSpec(memory_space=pltpu.HBM)] + [pl.BlockSpec(memory_space=pltpu.SMEM)] * 2,
        out_specs=[VSPEC] * 3,
        out_shape=[VMEM(flat.shape, F32)] + [jax.ShapeDtypeStruct(shape, F32)] * 2,
        scratch_shapes=[
            VMEM((frames, 2 * frames), F32),
            VMEM((LANES, 2 * LANES), F32),
            pltpu.SemaphoreType.DMA((rows // piece,)),
        ],
        compiler_params=params(),
        name="signal_grams",
    )(pltpu.with_memory_space_constraint(flat, pltpu.HBM), side, col)


def sweep(inner, image):
    count = inner.shape[0]
    blocks = count // SUB
    tiles = image.shape[1] // LANES
    a = [inner[SUB * i : SUB * (i + 1)] for i in range(blocks)]
    z = [
        [image[SUB * i : SUB * (i + 1), LANES * t : LANES * (t + 1)] for t in range(tiles)]
        for i in range(blocks)
    ]
    row = iota((SUB, LANES), 0)
    done = []
    for j in range(blocks):
        cols = [
            {i: jnp.broadcast_to(a[i][:, SUB * j + k : SUB * j + k + 1], (SUB, LANES)) for i in range(j, blocks)}
            for k in range(SUB)
        ]
        scale = jnp.zeros((SUB, LANES), F32)
        for k in range(SUB):
            inverse = jnp.broadcast_to((1.0 / cols[k][j])[k : k + 1], (SUB, LANES))
            scale = jnp.where(row == k, lax.rsqrt(cols[k][j]), scale)
            a_row = jnp.broadcast_to(a[j][k : k + 1], (SUB, LANES))
            z_row = [jnp.broadcast_to(t[k : k + 1], (SUB, LANES)) for t in z[j]]
            c_row = {
                q: jnp.broadcast_to(cols[q][j][k : k + 1], (SUB, LANES)) for q in range(k + 1, SUB)
            }
            for i in range(j, blocks):
                by = cols[k][i] * inverse
                if i == j:
                    by = jnp.where(row > k, by, 0.0)
                for q in range(k + 1, SUB):
                    cols[q][i] = cols[q][i] - by * c_row[q]
                if j + 1 < blocks:
                    a[i] = a[i] - by * a_row
                z[i] = [t - by * r for t, r in zip(z[i], z_row)]
        done.append([t * scale for t in z[j]])
    lines = [jnp.concatenate(d, axis=1) if tiles > 1 else d[0] for d in done]
    return jnp.concatenate(lines, axis=0) if blocks > 1 else lines[0]


def orthonormal(gram, start):
    def body(_, basis):
        image = mmf(basis, gram, NN)
        count = image.shape[0]
        padded = jnp.concatenate([image, jnp.zeros((LANES - count, image.shape[1]), F32)], axis=0)
        return sweep(mmf(image, padded, NT), image)

    return lax.fori_loop(0, ITERS, body, start)


def small_bases_kernel(
    kmax, cols, sends, mine_ref, other_ref, side_ref, sf_ref, ss_ref, rf_ref, rs_ref, frames_ref, spread_ref
):
    h = mine_ref.shape[0] - SUB
    left = side_ref[0] == 0
    mine, other = mine_ref[...], other_ref[...]
    first, last = jnp.where(left, mine, other), jnp.where(left, other, mine)
    gram_f = unpack(jnp.concatenate([first[:h], last[:h]], axis=1), jnp.concatenate([first[h:], last[h:]], axis=1))
    small = first[h:]
    lane = iota(small.shape, 1)
    gram_s = jnp.concatenate(
        [
            jnp.where(lane < sends, small, 0.0),
            jnp.where(lane < sends, pltpu.roll(small, LANES - sends, 1), 0.0),
            jnp.zeros((LANES - sends, LANES), F32),
        ],
        axis=0,
    )

    def body(_, bases):
        images = [mmf(basis, gram, NN) for basis, gram in zip(bases, (gram_f, gram_s))]
        inners = [
            mmf(i, jnp.concatenate([i, jnp.zeros((LANES - i.shape[0], i.shape[1]), F32)], axis=0), NT) for i in images
        ]
        return tuple(sweep(n, i) for n, i in zip(inners, images))

    basis_f, basis_s = lax.fori_loop(0, ITERS, body, (sf_ref[...], ss_ref[...]))
    frames_ref[...] = jnp.where(iota(basis_f.shape, 0) < rf_ref[0], basis_f, 0.0)
    basis_s = jnp.where(iota(basis_s.shape, 0) < rs_ref[0], basis_s, 0.0)
    pick = (iota((kmax, kmax * cols), 0) == iota((kmax, kmax * cols), 1) // cols).astype(F32)
    spread_ref[...] = mmf(basis_s, pick, TN)[:sends]


def small_bases(mine, other, side, start_frames, start_sends, rank_frames, rank_sends, cols):
    frames, tmax = start_frames.shape
    sends, kmax = start_sends.shape
    padded = jnp.pad(start_sends.T, ((0, 0), (0, LANES - sends)))
    smem = pl.BlockSpec(memory_space=pltpu.SMEM)
    return pl.pallas_call(
        functools.partial(small_bases_kernel, kmax, cols, sends),
        in_specs=[VSPEC, VSPEC, smem, VSPEC, VSPEC, smem, smem],
        out_specs=[VSPEC, VSPEC],
        out_shape=[jax.ShapeDtypeStruct((tmax, frames), F32), jax.ShapeDtypeStruct((sends, kmax * cols), F32)],
        compiler_params=params(),
        name="small_bases",
    )(mine, other, side, start_frames.T, padded, rank_frames, rank_sends)


def mixing(spread, cols):
    sends, wide = spread.shape
    tall = jnp.broadcast_to(spread[None], (cols, sends, wide)).reshape(cols * sends, wide)
    same = iota(tall.shape, 0) // sends == iota(tall.shape, 1) % cols
    return jnp.where(same, tall, 0.0)


def core_kernel(lanes, cols, per, x_ref, basis_ref, spread_ref, out_ref, held, mix_ref):
    tmax = basis_ref.shape[0]
    mix_ref[0], mix_ref[1] = split2(mixing(spread_ref[...], cols))
    bh, bl = split2(basis_ref[...])
    base = jnp.concatenate([bh, bl], axis=0)
    span = mix_ref.shape[1]

    def body(step, carry):
        his, los = [], []
        for q in range(per):
            at = pl.multiple_of((step * per + q) * span, span)
            xh, xl = split2(x_ref[pl.ds(at, span), :])
            both = mm(base, xh, NT)
            h, l = split2(both[:tmax] + (both[tmax:] + mm(bh, xl, NT)))
            his.append(h)
            los.append(l)
        rows = per * tmax
        stack = jnp.concatenate(his + los, axis=0)
        both = mm(stack, mix_ref[0], NN)
        c = both[:rows] + (both[rows:] + mm(stack[:rows], mix_ref[1], NN))
        for q in range(per):
            for h in range(c.shape[1] // lanes):
                held[step * per + q, h * tmax : (h + 1) * tmax] = c[
                    q * tmax : (q + 1) * tmax, h * lanes : (h + 1) * lanes
                ]
        return carry

    lax.fori_loop(0, held.shape[0] // per, body, 0)
    for r in range(held.shape[0]):
        out_ref[:, r, :] = held[r]


def project(flat, basis, spread, rows_dev, cols, lanes):
    tmax = basis.shape[0]
    sends, wide = spread.shape
    span = cols * sends
    per = 4 if rows_dev % 4 == 0 else 1
    high = wide * tmax // lanes
    return pl.pallas_call(
        functools.partial(core_kernel, lanes, cols, per),
        in_specs=[VSPEC] * 3,
        out_specs=VSPEC,
        out_shape=VMEM((high, rows_dev, lanes), F32),
        scratch_shapes=[VMEM((rows_dev, high, lanes), F32), VMEM((2, span, wide), BF16)],
        compiler_params=params(),
        name="project",
    )(flat, basis, spread)


def block_of(ref, j, g):
    part = ref[:, j, g]
    return part.reshape(part.shape[0] * part.shape[1], part.shape[2])


def row_gram_kernel(m_ref, col_ref, out_ref, *piece_refs):
    sections = m_ref.shape[1]
    for by, piece_ref in enumerate(piece_refs):
        to = target(col_ref[0], by, sections)
        for i in range(m_ref.shape[0]):
            for g in range(m_ref.shape[2]):
                piece_ref[i, g] = m_ref[i, to, g]
    total = None
    cross = None
    for j in range(m_ref.shape[1]):
        for g in range(m_ref.shape[2]):
            h, l = split2(block_of(m_ref, j, g))
            hh, hl = mm(h, h, NT), mm(h, l, NT)
            total = hh if total is None else total + hh
            cross = hl if cross is None else cross + hl
    put(out_ref, total + (cross + cross.T))


def put(ref, square):
    body, tail = pack(square)
    ref[: body.shape[0]] = body
    ref[body.shape[0] :] = tail


def get(ref):
    h = ref.shape[0] - SUB
    return unpack(ref[:h], ref[h:])


def row_gram(m, col):
    rows = m.shape[0] * m.shape[3]
    piece = jax.ShapeDtypeStruct((m.shape[0],) + m.shape[2:], F32)
    sections = m.shape[1]
    return pl.pallas_call(
        row_gram_kernel,
        in_specs=[VSPEC, pl.BlockSpec(memory_space=pltpu.SMEM)],
        out_specs=[VSPEC] * (1 + sections),
        out_shape=[jax.ShapeDtypeStruct((rows // 2 + SUB, rows), F32)] + [piece] * sections,
        compiler_params=params(),
        name="row_gram",
    )(m, col)


def second_kernel(cols, gram_ref, start_ref, col_ref, *refs):
    piece_refs = refs[:-3]
    basis_ref, second_ref, out_ref = refs[-3:]
    basis = orthonormal(get(gram_ref), start_ref[...])
    basis_ref[...] = basis
    uh, ul = split2(basis)
    twice = jnp.concatenate([uh, uh], axis=1)
    sections = len(piece_refs)
    low = piece_refs[0].shape[3] // cols
    total = None
    cross = None
    contract = (((0,), (1,)), ((), ()))
    for g in range(piece_refs[0].shape[1]):
        for by, piece_ref in enumerate(piece_refs):
            at = pl.multiple_of(source(col_ref[0], by, sections) * cols, cols)
            part = piece_ref[:, g]
            h, l = split2(part.reshape(part.shape[0] * part.shape[1], part.shape[2]))
            t = mm(jnp.concatenate([h, l], axis=0), twice, contract) + mm(h, ul, contract)
            for e in range(low):
                second_ref[g * low + e, pl.ds(at, cols)] = t[e * cols : (e + 1) * cols]
        for e in range(low):
            h, l = split2(second_ref[g * low + e])
            hh, hl = mm(h, h, NT), mm(h, l, NT)
            total = hh if total is None else total + hh
            cross = hl if cross is None else cross + hl
    put(out_ref, total + (cross + cross.T))


def second_stage(gram, start, col, pieces, cols):
    rows, kept = start.shape
    sections, groups, lanes = len(pieces), pieces[0].shape[1], pieces[0].shape[3]
    low = lanes // cols
    wide = sections * cols
    return pl.pallas_call(
        functools.partial(second_kernel, cols),
        in_specs=[VSPEC, VSPEC, pl.BlockSpec(memory_space=pltpu.SMEM)] + [VSPEC] * sections,
        out_specs=[VSPEC] * 3,
        out_shape=[
            jax.ShapeDtypeStruct((kept, rows), F32),
            jax.ShapeDtypeStruct((groups * low, wide, kept), F32),
            jax.ShapeDtypeStruct((wide // 2 + SUB, wide), F32),
        ],
        compiler_params=params(),
        name="second_stage",
    )(gram, start.T, col, *pieces)


def third_kernel(cols, gram_ref, start_ref, basis_ref, second_ref, out_ref):
    basis_c = orthonormal(get(gram_ref), start_ref[...])
    ph, pl_ = split2(mmf(basis_c, basis_c, TN))
    twice = jnp.concatenate([ph, ph], axis=1)
    rows_t = split2(basis_ref[...].T)
    sections = out_ref.shape[1]
    low = out_ref.shape[4] // cols
    for g in range(out_ref.shape[2]):
        kept = []
        for e in range(low):
            h, l = split2(second_ref[g * low + e])
            kept.append(split2(mm(twice, jnp.concatenate([h, l], axis=0), NN) + mm(pl_, h, NN)))
        for j in range(sections):
            part = [
                jnp.concatenate([k[w][j * cols : (j + 1) * cols] for k in kept], axis=0) for w in range(2)
            ]
            t = mm2(rows_t, part, NT)
            out_ref[:, j, g] = t.reshape(out_ref.shape[0], out_ref.shape[3], out_ref.shape[4])


def third_stage(gram, start, basis, second, shape, cols):
    return pl.pallas_call(
        functools.partial(third_kernel, cols),
        in_specs=[VSPEC] * 4,
        out_specs=VSPEC,
        out_shape=VMEM(shape, F32),
        compiler_params=params(),
        name="third_stage",
    )(gram, start.T, basis, second)


def expand_kernel(cols, per, x_ref, t_ref, basis_ref, spread_ref, out_ref, stage, held, mix_ref, base_ref, sems):
    tmax = basis_ref.shape[0]
    hi, lo = split2(mixing(spread_ref[...], cols))
    mix_ref[0], mix_ref[1] = hi.T, lo.T
    hi, lo = split2(basis_ref[...])
    for q, part in enumerate((hi, lo, hi)):
        base_ref[q * tmax : (q + 1) * tmax] = part
    for r in range(held.shape[0]):
        held[r] = t_ref[:, r, :]

    span = mix_ref.shape[2]
    rows = per * tmax
    steps = held.shape[0] // per

    def copy(step):
        at = pl.ds(pl.multiple_of(step * per * span, per * span), per * span)
        return pltpu.make_async_copy(stage.at[at, :], out_ref.at[at, :], sems.at[step])

    def body(step, carry):
        @pl.when(step > 0)
        def _():
            copy(step - 1).start()

        tiles = []
        for q in range(per):
            t = held[step * per + q]
            tiles.append(jnp.concatenate([t[h * tmax : (h + 1) * tmax] for h in range(t.shape[0] // tmax)], axis=1))
        hi, lo = split2(jnp.concatenate(tiles, axis=0))
        both = mm(jnp.concatenate([hi, lo], axis=0), mix_ref[0], NN)
        zh, zl = split2(both[:rows] + (both[rows:] + mm(hi, mix_ref[1], NN)))
        for q in range(per):
            h, l = zh[q * tmax : (q + 1) * tmax], zl[q * tmax : (q + 1) * tmax]
            tissue = mm(jnp.concatenate([h, h, l], axis=0), base_ref[...], TN)
            at = pl.multiple_of((step * per + q) * span, span)
            stage[pl.ds(at, span), :] = x_ref[pl.ds(at, span), :] - tissue
        return carry

    lax.fori_loop(0, steps, body, 0)
    copy(steps - 1).start()
    for step in range(steps):
        copy(step).wait()


def expand(flat, t, basis, spread, cols):
    frames = flat.shape[1]
    tmax = basis.shape[0]
    sends, wide = spread.shape
    high, rows_dev, lanes = t.shape
    span = cols * sends
    per = 2 if rows_dev % 2 == 0 else 1
    return pl.pallas_call(
        functools.partial(expand_kernel, cols, per),
        in_specs=[VSPEC] * 4,
        out_specs=pl.BlockSpec(memory_space=pltpu.HBM),
        out_shape=jax.ShapeDtypeStruct(flat.shape, F32),
        scratch_shapes=[
            VMEM(flat.shape, F32),
            VMEM((rows_dev, high, lanes), F32),
            VMEM((2, wide, span), BF16),
            VMEM((3 * tmax, frames), BF16),
            pltpu.SemaphoreType.DMA((rows_dev // per,)),
        ],
        compiler_params=params(),
        name="expand",
    )(flat, t, basis, spread)


def shifted(x, axis, by, size):
    return lax.ppermute(x, axis, [(i, target(i, by, size)) for i in range(size)])


def exchange_sum(x, axis, size, stride=1):
    total = x
    for by in range(stride, size, stride):
        total = total + shifted(x, axis, by, size)
    return total


def sum_all(x, rows, cols):
    x = exchange_sum(x, "col", cols)
    if rows % 2 or rows == 2:
        return exchange_sum(x, "row", rows)
    x = exchange_sum(x, "row", rows, 2)
    return x + lax.ppermute(x, "row", [(i, i ^ 1) for i in range(rows)])


def sum_halves(mine, other, rows, cols):
    pairs = [(i, i ^ 1) for i in range(rows)]
    mine = mine + lax.ppermute(other, "row", pairs)
    mine = exchange_sum(mine, "row", rows, 2)
    mine = exchange_sum(mine, "col", cols)
    return mine, lax.ppermute(mine, "row", pairs)


def local(rows, cols, signal, start_frames, start_sends, start_rows, start_cols, rank_frames, rank_sends):
    rows_dev, cols_dev, sends, frames = signal.shape
    kmax, tmax = start_sends.shape[1], start_frames.shape[1]
    devices = rows * cols
    flat = signal.reshape(-1, frames)
    side = (lax.axis_index("row") % 2).astype(jnp.int32).reshape(1)

    col = lax.axis_index("col").astype(jnp.int32).reshape(1)

    near, mine, other = signal_grams(flat, sends, side, col)
    mine, other = sum_halves(mine, other, rows, cols)
    basis, spread = small_bases(
        mine, other, side, start_frames, start_sends, rank_frames, rank_sends, cols_dev
    )

    low = min(LANES // cols_dev, kmax * tmax // devices, kmax)
    lanes = low * cols_dev
    near = in_vmem(near)
    core = project(near, basis, spread, rows_dev, cols_dev, lanes)
    groups = core.shape[0] // devices
    m = lax.all_to_all(core.reshape(rows, cols, groups, rows_dev, lanes), "row", 0, 0)

    gram_rows, *pieces = row_gram(m, col)
    pieces = [pieces[0]] + [shifted(piece, "col", by, cols) for by, piece in enumerate(pieces) if by]
    gram_rows = sum_all(gram_rows, rows, cols)
    basis_rows, second, gram_cols = second_stage(gram_rows, start_rows, col, pieces, cols_dev)
    gram_cols = sum_all(gram_cols, rows, cols)
    t = third_stage(gram_cols, start_cols, basis_rows, second, m.shape, cols_dev)

    t = t.reshape(devices, groups, rows_dev, lanes)
    t = lax.all_to_all(t, ("row", "col"), 0, 0).reshape(devices * groups, rows_dev, lanes)
    return expand(near, t, basis, spread, cols_dev).reshape(signal.shape)


def solution(mesh):
    rows, cols = mesh.shape["row"], mesh.shape["col"]
    return jax.shard_map(
        functools.partial(local, rows, cols),
        mesh=mesh,
        in_specs=(P("row", "col", None, None), P(), P(), P(), P(), P(), P()),
        out_specs=P("row", "col", None, None),
        check_vma=False,
    )
```
